512 devices in a mesh: gx: 32 (over z, y_lo, core), gy: 16 (over x, y_hi).
Axes of the slice: x: 4, y: 8 (y_hi: 4, y_lo: 2; y = y_hi * 2 + y_lo), z: 8, core: 2. Of those that a mesh axis runs over, the one named last changes fastest.
Arguments:
- potential: float32 [128, 256, 256], P('gx', 'gy'), may hold values from -0.2 to 1.2
- recovery: float32 [128, 256, 256], P('gx', 'gy'), may hold values from 0 to 1.5
- fiber_angles: float32 [2, 128, 256, 256], P(None, 'gx', 'gy'), may hold values from -3.140625 to 3.140625
- deform: float32 [9, 131072], P(None, ('gx', 'gy')), may hold values from -0.15 to 1.25, as said below
- elem_slot: int32 [32, 64, 64], P('gx', 'gy'), may hold values from 0 to 131071, as said below
Outputs:
- potential_next: float32 [128, 256, 256], P('gx', 'gy')
- recovery_next: float32 [128, 256, 256], P('gx', 'gy')
The draws below stay inside these ranges and needn't reach their ends.
Inputs may be any that keep to these rules, and one draw needn't show every extreme that they name: `elem_slot`: entries are distinct. Slot s lies on device s / 256 (rounded down) of gx+gy. The elements of one device's block along gx and gy lie in the slots of the devices with the same index along gx, exactly 16 of them in each. `deform`: components 0, 4 and 8 (the diagonal of F) lie in 0.8 to 1.25, the other six in -0.15 to 0.15.
All inputs are finite; a program needn't handle non-finite values.
Results may differ from the reference program's by a relative error of at most 0.0003.
Values sent between devices are 32-bit elements; how exact they have to be, the bound alone decides.
A program may use at most 64 MiB of HBM per device.

```python
import math
import jax
import jax.numpy as jnp
from jax import lax

RATIO = 4
KX = 1
KY = 4
NCZ = 64
NZ = 256
NX = 128
NY = 256
CB = 256
SHARE = 16
NE = 131072
N_GX = 32
N_GY = 16
DEVICES = 512


def draw_deform(key, part):
    diag_key = jax.random.fold_in(key, 21)
    off_key = jax.random.fold_in(key, 22)
    diagonal = jnp.exp(jax.random.uniform(diag_key, (3, NE), jnp.float32, math.log(0.8), math.log(1.25)))
    offside = jnp.clip(0.06 * jax.random.normal(off_key, (6, NE), jnp.float32), -0.15, 0.15)
    diagonal = jnp.clip(diagonal, 0.8, 1.25)
    rows = [diagonal[0], offside[0], offside[1], offside[2], diagonal[1], offside[3], offside[4], offside[5], diagonal[2]]
    return jnp.stack(rows).astype(jnp.float32)


def draw_elem_slot(key, part):
    block_keys = jax.random.split(jax.random.fold_in(key, 31), DEVICES)
    holder_keys = jax.random.split(jax.random.fold_in(key, 32), DEVICES)
    ranks = jax.vmap(lambda one_key: jax.random.permutation(one_key, CB))(block_keys).astype(jnp.int32)
    holding = jax.vmap(lambda one_key: jax.random.permutation(one_key, CB))(holder_keys).astype(jnp.int32)
    device_index = jnp.arange(DEVICES, dtype=jnp.int32)
    row_start = device_index // N_GY * N_GY
    column = device_index % N_GY
    holder = row_start[:, None] + ranks // SHARE
    position = column[:, None] * SHARE + ranks % SHARE
    local_slot = holding[holder, position]
    slots = holder * CB + local_slot
    grid = slots.reshape(N_GX, N_GY, KX, KY, NCZ).transpose(0, 2, 1, 3, 4).reshape(N_GX * KX, N_GY * KY, NCZ)
    return grid.astype(jnp.int32)


def block_scale(key, dims, shards, smallest, largest):
    def one(dim, parts):
        draws = jax.random.uniform(jax.random.fold_in(jax.random.fold_in(key, 6), dim), (parts,), jnp.float32, smallest / len(shards), largest / len(shards))
        return jnp.repeat(jnp.exp(draws), dims[dim] // parts).reshape((-1,) + (1,) * (len(dims) - dim - 1))

    level = one(*shards[0])
    for cut in shards[1:]:
        level = level * one(*cut)
    return level


def setup_inputs(seed: int = 0) -> dict:
    seeds = jax.random.split(jax.random.key(seed), 6)
    potential = jnp.clip(-0.2 + 1.4000001 * jax.random.uniform(seeds[0], (NX, NY, NZ), jnp.float32) ** block_scale(seeds[0], (NX, NY, NZ), ((0, 32), (1, 16)), -0.2, 0.2), -0.2, 1.2)
    recovery = jnp.clip(1.5 * jax.random.uniform(seeds[1], (NX, NY, NZ), jnp.float32) ** block_scale(seeds[1], (NX, NY, NZ), ((0, 32), (1, 16)), -0.2, 0.2), 0.0, 1.5)
    fiber_angles = jnp.clip(jax.random.uniform(seeds[2], (2, NX, NY, NZ), jnp.float32, -3.140625, 3.140625), -3.140625, 3.140625)
    deform = draw_deform(jax.random.fold_in(seeds[5], 71), 0)
    elem_slot = draw_elem_slot(jax.random.fold_in(seeds[5], 71), 0)
    return dict(potential=potential, recovery=recovery, fiber_angles=fiber_angles, deform=deform, elem_slot=elem_slot)


sigma_fiber = 1.0
sigma_cross = 0.3
time_step = 0.1
excite_gain = 8.0
excite_level = 0.15
stretch_gain = 10.0
stretch_reversal = 0.6
recover_rate = 0.5

def refine(padded, dim):
    inner_size = padded.shape[dim] - 2
    lower = lax.slice_in_dim(padded, 0, inner_size, axis=dim)
    middle = lax.slice_in_dim(padded, 1, inner_size + 1, axis=dim)
    upper = lax.slice_in_dim(padded, 2, inner_size + 2, axis=dim)
    pieces = []
    for position in range(RATIO):
        offset = (position + 0.5) / RATIO - 0.5
        weight = abs(offset)
        neighbor = lower if offset < 0 else upper
        pieces.append((1.0 - weight) * middle + weight * neighbor)
    stacked = jnp.stack(pieces, axis=dim + 1)
    new_shape = list(padded.shape)
    new_shape[dim] = inner_size * RATIO
    return stacked.reshape(new_shape)

def directions(angles):
    azimuth = angles[0]
    elevation = angles[1]
    return jnp.stack([jnp.cos(azimuth) * jnp.cos(elevation), jnp.sin(azimuth) * jnp.cos(elevation), jnp.sin(elevation)])

def tensors(field, fiber):
    entries = [field[number] for number in range(9)]

    def element(row_index, col_index):
        return entries[3 * (row_index % 3) + col_index % 3]
    cofactor = [[element(row_index + 1, col_index + 1) * element(row_index + 2, col_index + 2) - element(row_index + 1, col_index + 2) * element(row_index + 2, col_index + 1) for col_index in range(3)] for row_index in range(3)]
    determinant = element(0, 0) * cofactor[0][0] + element(0, 1) * cofactor[0][1] + element(0, 2) * cofactor[0][2]
    inverse = [[cofactor[col_index][row_index] / determinant for col_index in range(3)] for row_index in range(3)]
    stretched = [element(row_index, 0) * fiber[0] + element(row_index, 1) * fiber[1] + element(row_index, 2) * fiber[2] for row_index in range(3)]
    stretch = jnp.sqrt(stretched[0] * stretched[0] + stretched[1] * stretched[1] + stretched[2] * stretched[2])
    pulled = [inverse[row_index][0] * fiber[0] + inverse[row_index][1] * fiber[1] + inverse[row_index][2] * fiber[2] for row_index in range(3)]
    conduct = []
    for first_index, second_index in ((0, 0), (1, 1), (2, 2), (0, 1), (0, 2), (1, 2)):
        metric = inverse[first_index][0] * inverse[second_index][0] + inverse[first_index][1] * inverse[second_index][1] + inverse[first_index][2] * inverse[second_index][2]
        conduct.append(sigma_cross * metric + (sigma_fiber - sigma_cross) * pulled[first_index] * pulled[second_index])
    return (jnp.stack(conduct), stretch)

def close_faces(flux, dim, at_first, at_last):
    extent = flux.shape[dim]
    face_index = lax.broadcasted_iota(jnp.int32, flux.shape, dim)
    closed = (face_index == 0) & at_first | (face_index == extent - 1) & at_last
    return jnp.where(closed, jnp.zeros_like(flux), flux)

def divergence(potential_pad, tensor_pad, first_x, last_x, first_y, last_y):
    grad_x = (potential_pad[2:, :, :] - potential_pad[:-2, :, :]) * 0.5
    grad_y = (potential_pad[:, 2:, :] - potential_pad[:, :-2, :]) * 0.5
    grad_z = (potential_pad[:, :, 2:] - potential_pad[:, :, :-2]) * 0.5

    def face_mean(component, dim):
        inner = tensor_pad[component]
        if dim == 0:
            inner = inner[:, 1:-1, 1:-1]
        elif dim == 1:
            inner = inner[1:-1, :, 1:-1]
        else:
            inner = inner[1:-1, 1:-1, :]
        extent = inner.shape[dim]
        return (lax.slice_in_dim(inner, 1, extent, axis=dim) + lax.slice_in_dim(inner, 0, extent - 1, axis=dim)) * 0.5
    step_x = potential_pad[1:, 1:-1, 1:-1] - potential_pad[:-1, 1:-1, 1:-1]
    mean_y = (grad_y[1:, :, 1:-1] + grad_y[:-1, :, 1:-1]) * 0.5
    mean_z = (grad_z[1:, 1:-1, :] + grad_z[:-1, 1:-1, :]) * 0.5
    flux_x = face_mean(0, 0) * step_x + face_mean(3, 0) * mean_y + face_mean(4, 0) * mean_z
    flux_x = close_faces(flux_x, 0, first_x, last_x)
    step_y = potential_pad[1:-1, 1:, 1:-1] - potential_pad[1:-1, :-1, 1:-1]
    mean_x = (grad_x[:, 1:, 1:-1] + grad_x[:, :-1, 1:-1]) * 0.5
    mean_z = (grad_z[1:-1, 1:, :] + grad_z[1:-1, :-1, :]) * 0.5
    flux_y = face_mean(3, 1) * mean_x + face_mean(1, 1) * step_y + face_mean(5, 1) * mean_z
    flux_y = close_faces(flux_y, 1, first_y, last_y)
    step_z = potential_pad[1:-1, 1:-1, 1:] - potential_pad[1:-1, 1:-1, :-1]
    mean_x = (grad_x[:, 1:-1, 1:] + grad_x[:, 1:-1, :-1]) * 0.5
    mean_y = (grad_y[1:-1, :, 1:] + grad_y[1:-1, :, :-1]) * 0.5
    flux_z = face_mean(4, 2) * mean_x + face_mean(5, 2) * mean_y + face_mean(2, 2) * step_z
    flux_z = close_faces(flux_z, 2, True, True)
    return flux_x[1:] - flux_x[:-1] + (flux_y[:, 1:] - flux_y[:, :-1]) + (flux_z[:, :, 1:] - flux_z[:, :, :-1])

def update(voltage, recovery, divergent, stretch):
    current = excite_gain * voltage * (voltage - excite_level) * (voltage - 1.0) + voltage * recovery
    current = current + stretch_gain * jnp.maximum(stretch - 1.0, 0.0) * (voltage - stretch_reversal)
    voltage_next = voltage + time_step * (divergent - current)
    recovery_next = recovery + time_step * recover_rate * (-recovery - excite_gain * voltage * (voltage - excite_level - 1.0))
    return (voltage_next, recovery_next)

def reference(potential, recovery, fiber_angles, deform, elem_slot):
    coarse = deform[:, elem_slot]
    coarse = jnp.pad(coarse, ((0, 0), (1, 1), (1, 1), (1, 1)), mode='edge')
    along_x = refine(coarse, 1)
    along_x = jnp.pad(along_x, ((0, 0), (1, 1), (0, 0), (0, 0)), mode='edge')
    angles_pad = jnp.pad(fiber_angles, ((0, 0), (1, 1), (0, 0), (0, 0)), mode='edge')
    potential_all = jnp.pad(potential, 1, mode='edge')
    width = NX // N_GX

    def slab(index):
        start = (index * width).astype(jnp.int32)
        segment = lax.dynamic_slice_in_dim(along_x, start, width + 2, axis=1)
        fine_field = refine(refine(segment, 2), 3)
        angles = lax.dynamic_slice_in_dim(angles_pad, start, width + 2, axis=1)
        conduct, stretch = tensors(fine_field, directions(angles))
        tensor_pad = jnp.pad(conduct, ((0, 0), (0, 0), (1, 1), (1, 1)), mode='edge')
        potential_pad = lax.dynamic_slice_in_dim(potential_all, start, width + 2, axis=0)
        divergent = divergence(potential_pad, tensor_pad, index == 0, index == N_GX - 1, True, True)
        voltage = lax.dynamic_slice_in_dim(potential, start, width, axis=0)
        resting = lax.dynamic_slice_in_dim(recovery, start, width, axis=0)
        return update(voltage, resting, divergent, stretch[1:-1])
    voltage_next, recovery_next = lax.map(slab, jnp.arange(N_GX, dtype=jnp.int32))
    return (voltage_next.reshape(NX, NY, NZ), recovery_next.reshape(NX, NY, NZ))
```

```python
import jax
import jax.numpy as jnp
from jax import lax
from jax.experimental import pallas as pl
from jax.experimental.pallas import tpu as pltpu
from jax.sharding import PartitionSpec as P

sigma_fiber = 1.0
sigma_cross = 0.3
time_step = 0.1
excite_gain = 8.0
excite_level = 0.15
stretch_gain = 10.0
stretch_reversal = 0.6
recover_rate = 0.5

MESH = pl.DeviceIdType.MESH
F32 = jnp.float32
BF16 = jnp.bfloat16

ROWS = 104
LAST = 96


def sin_cos(angle):
    half = 0.5 * angle
    sq = half * half
    s = -2.5052108e-08
    for c in (2.7557319e-06, -1.9841270e-04, 8.3333333e-03, -1.6666667e-01, 1.0):
        s = s * sq + c
    s = s * half
    c2 = 2.0876757e-09
    for c in (-2.7557319e-07, 2.4801587e-05, -1.3888889e-03, 4.1666667e-02, -0.5, 1.0):
        c2 = c2 * sq + c
    return 2.0 * s * c2, 1.0 - 2.0 * s * s


def fibers(azimuth, elevation):
    sin_a, cos_a = sin_cos(azimuth)
    sin_e, cos_e = sin_cos(elevation)
    return cos_a * cos_e, sin_a * cos_e, sin_e


def tensor_rows(f, fiber, want_stretch):
    def el(i, j):
        return f[3 * (i % 3) + j % 3]

    cof = [
        [el(i + 1, j + 1) * el(i + 2, j + 2) - el(i + 1, j + 2) * el(i + 2, j + 1) for j in range(3)]
        for i in range(3)
    ]
    det = el(0, 0) * cof[0][0] + el(0, 1) * cof[0][1] + el(0, 2) * cof[0][2]
    inv = 1.0 / det
    scale = inv * inv
    stretch = None
    if want_stretch:
        st = [el(i, 0) * fiber[0] + el(i, 1) * fiber[1] + el(i, 2) * fiber[2] for i in range(3)]
        stretch = jnp.sqrt(st[0] * st[0] + st[1] * st[1] + st[2] * st[2])
    pulled = [cof[0][i] * fiber[0] + cof[1][i] * fiber[1] + cof[2][i] * fiber[2] for i in range(3)]
    out = []
    for a, b in ((0, 0), (1, 1), (2, 2), (0, 1), (0, 2), (1, 2)):
        metric = cof[0][a] * cof[0][b] + cof[1][a] * cof[1][b] + cof[2][a] * cof[2][b]
        out.append(
            (sigma_cross * metric + (sigma_fiber - sigma_cross) * pulled[a] * pulled[b]) * scale
        )
    return out, stretch


def kernel(
    n_x, n_y, split, order,
    pot_in, rec_in, ang_in, def_in, slot_in, pot_out, rec_out,
    pot, rec, ang, dfm, slot, ag8, ag1, ysend, yrecv, srecv, xpot, xang, xcor, s8, s1,
    fib, crs, fine, con, stretch, vh, onew, onev,
    in_sem, out_sem, ag_send, ag_recv, y_send, y_recv, x_send, x_recv, c_send, c_recv,
):
    gx = lax.axis_index("gx")
    gy = lax.axis_index("gy")
    up_x, down_x = lax.rem(gx + 1, n_x), lax.rem(gx + n_x - 1, n_x)
    up_y, down_y = lax.rem(gy + 1, n_y), lax.rem(gy + n_y - 1, n_y)
    outer, inner = split
    my_o, my_i = lax.div(gy, inner), lax.rem(gy, inner)

    def peer(number):
        step_o, step_i = number // inner, number % inner
        return lax.rem(my_o + step_o, outer) * inner + lax.rem(my_i + step_i, inner)

    barrier = pltpu.get_barrier_semaphore()
    for number in order:
        pl.semaphore_signal(barrier, inc=1, device_id=(gx, peer(number)), device_id_type=MESH)
    for other in (up_x, down_x):
        pl.semaphore_signal(barrier, inc=1, device_id=(other, gy), device_id_type=MESH)

    loads = [
        pltpu.make_async_copy(src, dst, in_sem.at[i])
        for i, (src, dst) in enumerate(
            ((def_in, dfm), (slot_in, slot), (pot_in, pot), (ang_in, ang), (rec_in, rec))
        )
    ]
    for load in loads:
        load.start()
    loads[0].wait()
    ag8[0] = dfm[0:8]
    ag1[0] = dfm[8:9]
    loads[1].wait()
    loads[2].wait()
    loads[3].wait()
    for side, row in ((0, 0), (1, 15)):
        ysend[side, 0:4] = pot[:, row, :]
        ysend[side, 4:8] = ang[0, :, row, :]
        ysend[side, 8:12] = ang[1, :, row, :]

    pl.semaphore_wait(barrier, n_y + 1)

    sends = []

    def send(src, dst, send_sem, recv_sem, device):
        copy = pltpu.make_async_remote_copy(
            src_ref=src, dst_ref=dst, send_sem=send_sem, recv_sem=recv_sem,
            device_id=device, device_id_type=MESH,
        )
        copy.start()
        sends.append(copy)
        return copy

    gathers = []
    for number in order:
        device = (gx, peer(number))
        gathers.append(send(ag8.at[0], ag8.at[number], ag_send.at[0, number], ag_recv.at[0, number], device))
        gathers.append(send(ag1.at[0], ag1.at[number], ag_send.at[1, number], ag_recv.at[1, number], device))
    halos = []
    for side, device in ((0, (gx, down_y)), (1, (gx, up_y))):
        halos.append(send(slot, srecv.at[1 - side], y_send.at[0, side], y_recv.at[0, side], device))
        halos.append(send(ysend.at[side], yrecv.at[1 - side], y_send.at[1, side], y_recv.at[1, side], device))
    planes = []
    for side, device in ((0, (down_x, gy)), (1, (up_x, gy))):
        planes.append(send(pot.at[3 * side], xpot.at[1 - side], x_send.at[0, side], x_recv.at[0, side], device))
        for which in range(2):
            planes.append(
                send(
                    ang.at[which, 3 * side], xang.at[1 - side, which],
                    x_send.at[1 + which, side], x_recv.at[1 + which, side], device,
                )
            )

    loads[4].wait()
    for x in range(4):
        v, w = pot[x], rec[x]
        onew[x] = w + time_step * recover_rate * (
            -w - excite_gain * v * (v - excite_level - 1.0)
        )
        f = fibers(ang[0, x], ang[1, x])
        for i in range(3):
            fib[i, 16 * (x + 1) : 16 * (x + 2)] = f[i]
    rec_store = pltpu.make_async_copy(onew, rec_out, out_sem.at[0])
    rec_store.start()

    k_iota = lax.broadcasted_iota(jnp.int32, (128, 256), 0) & 63
    z_iota = lax.broadcasted_iota(jnp.int32, (128, 256), 1)
    place = jnp.clip((z_iota.astype(F32) + 0.5) * 0.25 - 0.5, 0.0, 63.0)
    hat = jnp.maximum(1.0 - jnp.abs(place - k_iota.astype(F32)), 0.0).astype(BF16)

    for copy in halos:
        copy.wait_recv()
    corners = []
    for side, device in ((0, (down_x, gy)), (1, (up_x, gy))):
        for which in range(2):
            corners.append(
                send(
                    yrecv.at[which, 0:8], xcor.at[1 - side, which],
                    x_send.at[3 + which, side], x_recv.at[3 + which, side], device,
                )
            )
    azimuth = jnp.concatenate([yrecv[0, 4:8], yrecv[1, 4:8]], axis=0)
    elevation = jnp.concatenate([yrecv[0, 8:12], yrecv[1, 8:12]], axis=0)
    f = fibers(azimuth, elevation)
    for i in range(3):
        fib[i, LAST : LAST + 8] = f[i]

    mine = slot[...]
    below = jnp.where(gy == 0, mine[0:1], srecv[0, 3:4])
    above = jnp.where(gy == n_y - 1, mine[3:4], srecv[1, 0:1])
    wanted = jnp.concatenate(
        [piece for row in (below, mine[0:1], mine[1:2], mine[2:3], mine[3:4], above) for piece in (row, row)],
        axis=1,
    )
    local = wanted & 255
    holder = (wanted >> 8) & (n_y - 1)
    from_o = (my_o - (holder >> (inner.bit_length() - 1))) & (outer - 1)
    from_i = (my_i - (holder & (inner - 1))) & (inner - 1)
    source = from_o * inner + from_i
    hot = jnp.where(
        lax.broadcasted_iota(jnp.int32, (256, 768), 0) == local, 1.0, 0.0
    ).astype(BF16)

    for copy in gathers:
        copy.wait_recv()
    d8 = ag8[...].reshape(n_y * 8, 256)
    d1 = ag1[...].reshape(n_y, 256)
    both = jnp.concatenate([d8, d1], axis=0)
    high = both.astype(BF16)
    low = (both - high.astype(F32)).astype(BF16)
    chosen = jnp.dot(high, hot, preferred_element_type=F32) + jnp.dot(
        low, hot, preferred_element_type=F32
    )
    total = jnp.zeros((8, 768), F32)
    for number in range(n_y):
        total = total + jnp.where(source == number, chosen[8 * number : 8 * number + 8], 0.0)
    s8[0] = total
    last = chosen[8 * n_y : 9 * n_y]
    s1[0] = jnp.sum(
        jnp.where(lax.broadcasted_iota(jnp.int32, (n_y, 768), 0) == source, last, 0.0),
        axis=0, keepdims=True,
    )
    coarse = []
    for side, device in ((0, (down_x, gy)), (1, (up_x, gy))):
        coarse.append(send(s8.at[0], s8.at[2 - side], c_send.at[0, side], c_recv.at[0, side], device))
        coarse.append(send(s1.at[0], s1.at[2 - side], c_send.at[1, side], c_recv.at[1, side], device))

    for copy in planes:
        copy.wait_recv()
    for side, start in ((0, 0), (1, 80)):
        f = fibers(xang[side, 0], xang[side, 1])
        for i in range(3):
            fib[i, start : start + 16] = f[i]
    for copy in corners:
        copy.wait_recv()
    first_x, last_x, first_y, last_y = gx == 0, gx == n_x - 1, gy == 0, gy == n_y - 1
    volt = [jnp.where(first_x, pot[0], xpot[0])]
    volt += [pot[x] for x in range(4)]
    volt += [jnp.where(last_x, pot[3], xpot[1])]
    for which, row, outside in ((0, 0, first_y), (1, 15, last_y)):
        ring = [
            jnp.where(first_x, yrecv[which, 0:1], xcor[0, which, 3:4]),
            yrecv[which, 0:1], yrecv[which, 1:2], yrecv[which, 2:3], yrecv[which, 3:4],
            jnp.where(last_x, yrecv[which, 3:4], xcor[1, which, 0:1]),
        ]
        for p in range(6):
            vh[which, p : p + 1] = jnp.where(outside, volt[p][row : row + 1], ring[p])

    for copy in coarse:
        copy.wait_recv()
    sub = lax.broadcasted_iota(jnp.int32, (8, 128), 0)

    def hat_rows(start, element):
        t = (sub.astype(F32) + (start + 0.5)) * 0.25 - 0.5
        return jnp.maximum(1.0 - jnp.abs(t - element), 0.0)

    tile0 = [hat_rows(0, e - 1) for e in range(4)]
    tile1 = [hat_rows(8, e + 1) for e in range(4)]
    t = ((sub & 3).astype(F32) + 0.5) * 0.25 - 0.5
    cross = [jnp.maximum(1.0 - jnp.abs(t - (e - 1)), 0.0) for e in range(3)]
    low_half = sub < 4
    for k in range(9):
        tiles0, tiles1, beside = [], [], []
        for which in (1, 0, 2):
            rows = []
            for e in range(6):
                lanes = slice(128 * e, 128 * e + 128)
                row = s8[which, k : k + 1, lanes] if k < 8 else s1[which, :, lanes]
                if which == 1:
                    own = s8[0, k : k + 1, lanes] if k < 8 else s1[0, :, lanes]
                    row = jnp.where(first_x, own, row)
                if which == 2:
                    own = s8[0, k : k + 1, lanes] if k < 8 else s1[0, :, lanes]
                    row = jnp.where(last_x, own, row)
                rows.append(jnp.broadcast_to(row, (8, 128)))
            tiles0.append(sum(tile0[i] * rows[i] for i in range(4)))
            tiles1.append(sum(tile1[i] * rows[i + 2] for i in range(4)))
            beside.append(
                jnp.where(low_half, 0.625 * rows[0] + 0.375 * rows[1], 0.625 * rows[5] + 0.375 * rows[4])
            )
        base = ROWS * k
        for p, (a, b, c) in enumerate(
            (
                (0.625, 0.375, 0.0), (0.375, 0.625, 0.0), (0.125, 0.875, 0.0),
                (0.0, 0.875, 0.125), (0.0, 0.625, 0.375), (0.0, 0.375, 0.625),
            )
        ):
            for half, tiles in ((0, tiles0), (8, tiles1)):
                if c == 0.0:
                    value = a * tiles[0] + b * tiles[1]
                else:
                    value = b * tiles[1] + c * tiles[2]
                crs[base + 16 * p + half : base + 16 * p + half + 8] = value
        crs[base + LAST : base + LAST + 8] = (
            cross[0] * beside[0] + cross[1] * beside[1] + cross[2] * beside[2]
        )
    c = crs[...]
    rest = c - c.astype(BF16).astype(F32)
    left = lax.broadcasted_iota(jnp.int32, c.shape, 1) < 64
    fine[...] = jnp.dot(
        jnp.where(left, c, rest).astype(BF16), hat, preferred_element_type=F32
    )

    for tile in range(13):
        at = 8 * tile
        f = [fine[ROWS * k + at : ROWS * k + at + 8] for k in range(9)]
        fiber = [fib[i, at : at + 8] for i in range(3)]
        own = 2 <= tile < 10
        d, s = tensor_rows(f, fiber, own)
        for i in range(6):
            con[i, at : at + 8] = d[i]
        if own:
            stretch[at - 16 : at - 8] = s

    row_iota = lax.broadcasted_iota(jnp.int32, (16, 256), 0)
    lane = lax.broadcasted_iota(jnp.int32, (16, 256), 1)

    def from_below(a, edge):
        return jnp.where(row_iota == 0, edge, pltpu.roll(a, 1, 0))

    def from_above(a, edge):
        return jnp.where(row_iota == 15, edge, pltpu.roll(a, 15, 0))

    def z_slope(v):
        n = v.shape[0]
        at = lax.broadcasted_iota(jnp.int32, (n, 256), 1)
        after = jnp.where(at == 255, v, pltpu.roll(v, 255, 1))
        before = jnp.where(at == 0, v, pltpu.roll(v, 1, 1))
        return after - before

    def flux(d1, step, d2, s2, d3, s3):
        return 0.5 * (d1 * step + 0.25 * (d2 * s2 + d3 * s3))

    XX, YY, ZZ, XY, XZ, YZ = range(6)
    slope_y = [from_above(volt[p], vh[1, p : p + 1]) - from_below(volt[p], vh[0, p : p + 1]) for p in range(6)]
    slope_z = [z_slope(volt[p]) for p in range(6)]
    edge_z = [z_slope(vh[which]) for which in range(2)]

    def plane(i, p):
        return con[i, 16 * p : 16 * p + 16]

    flux_x = []
    for p in range(5):
        value = flux(
            plane(XX, p) + plane(XX, p + 1), volt[p + 1] - volt[p],
            plane(XY, p) + plane(XY, p + 1), slope_y[p] + slope_y[p + 1],
            plane(XZ, p) + plane(XZ, p + 1), slope_z[p] + slope_z[p + 1],
        )
        if p == 0:
            value = jnp.where(first_x, 0.0, value)
        if p == 4:
            value = jnp.where(last_x, 0.0, value)
        flux_x.append(value)
    for x in range(4):
        p = x + 1
        v = volt[p]
        slope_x = volt[p + 1] - volt[p - 1]
        d_xy, d_yy, d_yz = plane(XY, p), plane(YY, p), plane(YZ, p)
        faces = []
        for which, shift in ((0, from_below), (1, from_above)):
            row = LAST + 4 * which + x
            step = shift(v, vh[which, p : p + 1])
            step = v - step if which == 0 else step - v
            faces.append(
                flux(
                    d_yy + shift(d_yy, con[YY, row : row + 1]), step,
                    d_xy + shift(d_xy, con[XY, row : row + 1]),
                    slope_x + shift(slope_x, vh[which, p + 1 : p + 2] - vh[which, p - 1 : p]),
                    d_yz + shift(d_yz, con[YZ, row : row + 1]),
                    slope_z[p] + shift(slope_z[p], edge_z[which][p : p + 1]),
                )
            )
        faces[0] = jnp.where((row_iota == 0) & first_y, 0.0, faces[0])
        faces[1] = jnp.where((row_iota == 15) & last_y, 0.0, faces[1])

        def onward(a):
            return pltpu.roll(a, 255, 1)

        d_xz, d_zz = plane(XZ, p), plane(ZZ, p)
        upper = flux(
            d_zz + onward(d_zz), onward(v) - v,
            d_xz + onward(d_xz), slope_x + onward(slope_x),
            d_yz + onward(d_yz), slope_y[p] + onward(slope_y[p]),
        )
        upper = jnp.where(lane == 255, 0.0, upper)
        divergent = (
            flux_x[p] - flux_x[p - 1] + (faces[1] - faces[0]) + (upper - pltpu.roll(upper, 1, 1))
        )
        w = rec[x]
        current = excite_gain * v * (v - excite_level) * (v - 1.0) + v * w
        current = current + stretch_gain * jnp.maximum(stretch[16 * x : 16 * x + 16] - 1.0, 0.0) * (
            v - stretch_reversal
        )
        onev[x] = v + time_step * (divergent - current)
    pot_store = pltpu.make_async_copy(onev, pot_out, out_sem.at[1])
    pot_store.start()
    for copy in sends:
        copy.wait_send()
    rec_store.wait()
    pot_store.wait()


def make_local(n_x, n_y):
    split = (4, 4) if n_y == 16 else (n_y // 2, 2)
    outer, inner = split

    def reach(number):
        o, i = number // inner, number % inner
        return min(o, outer - o) + 2 * min(i, inner - i)

    order = sorted(range(1, n_y), key=lambda number: -reach(number))

    def local(potential, recovery, fiber_angles, deform, elem_slot):
        anywhere = pl.BlockSpec(memory_space=pl.ANY)
        cells = (4, 16, 256)
        dma = pltpu.SemaphoreType.DMA
        call = pl.pallas_call(
            lambda *refs: kernel(n_x, n_y, split, order, *refs),
            out_shape=(jax.ShapeDtypeStruct(cells, F32),) * 2,
            in_specs=[anywhere] * 5,
            out_specs=(anywhere, anywhere),
            scratch_shapes=[
                pltpu.VMEM(cells, F32),
                pltpu.VMEM(cells, F32),
                pltpu.VMEM((2,) + cells, F32),
                pltpu.VMEM((9, 256), F32),
                pltpu.VMEM((4, 64), jnp.int32),
                pltpu.VMEM((n_y, 8, 256), F32),
                pltpu.VMEM((n_y, 1, 256), F32),
                pltpu.VMEM((2, 16, 256), F32),
                pltpu.VMEM((2, 16, 256), F32),
                pltpu.VMEM((2, 4, 64), jnp.int32),
                pltpu.VMEM((2, 16, 256), F32),
                pltpu.VMEM((2, 2, 16, 256), F32),
                pltpu.VMEM((2, 2, 8, 256), F32),
                pltpu.VMEM((3, 8, 768), F32),
                pltpu.VMEM((3, 1, 768), F32),
                pltpu.VMEM((3, ROWS, 256), F32),
                pltpu.VMEM((9 * ROWS, 128), F32),
                pltpu.VMEM((9 * ROWS, 256), F32),
                pltpu.VMEM((6, ROWS, 256), F32),
                pltpu.VMEM((64, 256), F32),
                pltpu.VMEM((2, 8, 256), F32),
                pltpu.VMEM(cells, F32),
                pltpu.VMEM(cells, F32),
                dma((5,)),
                dma((2,)),
                dma((2, n_y)),
                dma((2, n_y)),
                dma((2, 2)),
                dma((2, 2)),
                dma((5, 2)),
                dma((5, 2)),
                dma((2, 2)),
                dma((2, 2)),
            ],
            compiler_params=pltpu.CompilerParams(collective_id=0, has_side_effects=True),
            name="step",
        )
        return call(potential, recovery, fiber_angles, deform, elem_slot.reshape(4, 64))

    return local


def solution(mesh):
    placed = (
        P("gx", "gy", None),
        P("gx", "gy", None),
        P(None, "gx", "gy", None),
        P(None, ("gx", "gy")),
        P("gx", "gy", None),
    )
    return jax.shard_map(
        make_local(mesh.shape["gx"], mesh.shape["gy"]),
        mesh=mesh,
        in_specs=placed,
        out_specs=(P("gx", "gy", None), P("gx", "gy", None)),
        check_vma=False,
    )
```

```python
import jax
import jax.numpy as jnp
from jax import lax
from jax.experimental import pallas as pl
from jax.experimental.pallas import tpu as pltpu
from jax.sharding import PartitionSpec as P

sigma_fiber = 1.0
sigma_cross = 0.3
time_step = 0.1
excite_gain = 8.0
excite_level = 0.15
stretch_gain = 10.0
stretch_reversal = 0.6
recover_rate = 0.5

MESH = pl.DeviceIdType.MESH
F32 = jnp.float32
BF16 = jnp.bfloat16

ROWS = 104
LAST = 96


def sin_cos(angle):
    half = 0.5 * angle
    sq = half * half
    s = -2.5052108e-08
    for c in (2.7557319e-06, -1.9841270e-04, 8.3333333e-03, -1.6666667e-01, 1.0):
        s = s * sq + c
    s = s * half
    c2 = 2.0876757e-09
    for c in (-2.7557319e-07, 2.4801587e-05, -1.3888889e-03, 4.1666667e-02, -0.5, 1.0):
        c2 = c2 * sq + c
    return 2.0 * s * c2, 1.0 - 2.0 * s * s


def fibers(azimuth, elevation):
    sin_a, cos_a = sin_cos(azimuth)
    sin_e, cos_e = sin_cos(elevation)
    return cos_a * cos_e, sin_a * cos_e, sin_e


def tensor_rows(f, fiber, want_stretch):
    def el(i, j):
        return f[3 * (i % 3) + j % 3]

    cof = [
        [el(i + 1, j + 1) * el(i + 2, j + 2) - el(i + 1, j + 2) * el(i + 2, j + 1) for j in range(3)]
        for i in range(3)
    ]
    det = el(0, 0) * cof[0][0] + el(0, 1) * cof[0][1] + el(0, 2) * cof[0][2]
    inv = 1.0 / det
    scale = inv * inv
    stretch = None
    if want_stretch:
        st = [el(i, 0) * fiber[0] + el(i, 1) * fiber[1] + el(i, 2) * fiber[2] for i in range(3)]
        stretch = jnp.sqrt(st[0] * st[0] + st[1] * st[1] + st[2] * st[2])
    pulled = [cof[0][i] * fiber[0] + cof[1][i] * fiber[1] + cof[2][i] * fiber[2] for i in range(3)]
    out = []
    for a, b in ((0, 0), (1, 1), (2, 2), (0, 1), (0, 2), (1, 2)):
        metric = cof[0][a] * cof[0][b] + cof[1][a] * cof[1][b] + cof[2][a] * cof[2][b]
        out.append(
            (sigma_cross * metric + (sigma_fiber - sigma_cross) * pulled[a] * pulled[b]) * scale
        )
    return out, stretch


def kernel(
    n_x, n_y, split, order,
    pot_in, rec_in, ang_in, def_in, slot_in, pot_out, rec_out,
    pot, rec, ang, dfm, slot, ag8, ag1, ysend, yrecv, srecv, xpot, xang, xcor, s8, s1,
    fib, crs, fine, con, stretch, vh, onew, onev,
    in_sem, out_sem, ag_send, ag_recv, y_send, y_recv, x_send, x_recv, c_send, c_recv,
):
    gx = lax.axis_index("gx")
    gy = lax.axis_index("gy")
    first_x, last_x, first_y, last_y = gx == 0, gx == n_x - 1, gy == 0, gy == n_y - 1
    x_sides = ((jnp.logical_not(first_x), (gx - 1, gy), 0), (jnp.logical_not(last_x), (gx + 1, gy), 3))
    y_sides = ((jnp.logical_not(first_y), (gx, gy - 1), 0), (jnp.logical_not(last_y), (gx, gy + 1), 15))
    outer, inner = split
    my_o, my_i = lax.div(gy, inner), lax.rem(gy, inner)

    def peer(number):
        step_o, step_i = number // inner, number % inner
        return lax.rem(my_o + step_o, outer) * inner + lax.rem(my_i + step_i, inner)

    loads = [
        pltpu.make_async_copy(src, dst, in_sem.at[i])
        for i, (src, dst) in enumerate(
            ((def_in, dfm), (slot_in, slot), (pot_in, pot), (ang_in, ang), (rec_in, rec))
        )
    ]
    loads[0].start()
    barrier = pltpu.get_barrier_semaphore()
    for number in order:
        pl.semaphore_signal(barrier, inc=1, device_id=(gx, peer(number)), device_id_type=MESH)
    for there, device, _ in x_sides:

        @pl.when(there)
        def _(device=device):
            pl.semaphore_signal(barrier, inc=1, device_id=device, device_id_type=MESH)

    for load in loads[1:]:
        load.start()
    loads[0].wait()
    ag8[0] = dfm[0:8]
    ag1[0] = dfm[8:9]
    pl.semaphore_wait(barrier, n_y - 1 + jnp.where(first_x, 0, 1) + jnp.where(last_x, 0, 1))

    def remote(src, dst, send_sem, recv_sem, device):
        return pltpu.make_async_remote_copy(
            src_ref=src, dst_ref=dst, send_sem=send_sem, recv_sem=recv_sem,
            device_id=device, device_id_type=MESH,
        )

    def send(there, copies):
        @pl.when(there)
        def _():
            for copy in copies:
                copy.start()

    def arrived(there, copies, otherwise):
        @pl.when(there)
        def _():
            for copy in copies:
                copy.wait_recv()

        @pl.when(jnp.logical_not(there))
        def _():
            otherwise()

    def sent(there, copies):
        @pl.when(there)
        def _():
            for copy in copies:
                copy.wait_send()

    gathers = []
    for number in order:
        device = (gx, peer(number))
        gathers += [
            remote(ag8.at[0], ag8.at[number], ag_send.at[0, number], ag_recv.at[0, number], device),
            remote(ag1.at[0], ag1.at[number], ag_send.at[1, number], ag_recv.at[1, number], device),
        ]
        for copy in gathers[-2:]:
            copy.start()
    loads[1].wait()
    loads[2].wait()
    loads[3].wait()
    halos, planes, corners, coarse = [], [], [], []
    for side, (there, device, row) in enumerate(y_sides):
        ysend[side, 0:4] = pot[:, row, :]
        ysend[side, 4:8] = ang[0, :, row, :]
        ysend[side, 8:12] = ang[1, :, row, :]
        halos.append(
            [
                remote(slot, srecv.at[1 - side], y_send.at[0, side], y_recv.at[0, 1 - side], device),
                remote(ysend.at[side], yrecv.at[1 - side], y_send.at[1, side], y_recv.at[1, 1 - side], device),
            ]
        )
    for side, (there, device, x) in enumerate(x_sides):
        planes.append(
            [remote(pot.at[x], xpot.at[1 - side], x_send.at[0, side], x_recv.at[0, 1 - side], device)]
            + [
                remote(
                    ang.at[which, x], xang.at[1 - side, which],
                    x_send.at[1 + which, side], x_recv.at[1 + which, 1 - side], device,
                )
                for which in range(2)
            ]
        )
        corners.append(
            [
                remote(
                    yrecv.at[which, 0:8], xcor.at[1 - side, which],
                    x_send.at[3 + which, side], x_recv.at[3 + which, 1 - side], device,
                )
                for which in range(2)
            ]
        )
        coarse.append(
            [
                remote(s8.at[0], s8.at[2 - side], c_send.at[0, side], c_recv.at[0, 1 - side], device),
                remote(s1.at[0], s1.at[2 - side], c_send.at[1, side], c_recv.at[1, 1 - side], device),
            ]
        )
    for (there, _, _), copies in zip(x_sides, planes):
        send(there, copies)
    for (there, _, _), copies in zip(y_sides, halos):
        send(there, copies)

    loads[4].wait()
    for x in range(4):
        v, w = pot[x], rec[x]
        onew[x] = w + time_step * recover_rate * (
            -w - excite_gain * v * (v - excite_level - 1.0)
        )
        f = fibers(ang[0, x], ang[1, x])
        for i in range(3):
            fib[i, 16 * (x + 1) : 16 * (x + 2)] = f[i]
    rec_store = pltpu.make_async_copy(onew, rec_out, out_sem.at[0])
    rec_store.start()

    k_iota = lax.broadcasted_iota(jnp.int32, (128, 256), 0) & 63
    z_iota = lax.broadcasted_iota(jnp.int32, (128, 256), 1)
    place = jnp.clip((z_iota.astype(F32) + 0.5) * 0.25 - 0.5, 0.0, 63.0)
    hat = jnp.maximum(1.0 - jnp.abs(place - k_iota.astype(F32)), 0.0).astype(BF16)

    for side, (there, _, row) in enumerate(y_sides):

        def own_row(side=side, row=row):
            yrecv[side, 0:12] = ysend[side, 0:12]
            srecv[side] = slot[...]

        arrived(there, halos[1 - side], own_row)
    for (there, _, _), copies in zip(x_sides, corners):
        send(there, copies)
    azimuth = jnp.concatenate([yrecv[0, 4:8], yrecv[1, 4:8]], axis=0)
    elevation = jnp.concatenate([yrecv[0, 8:12], yrecv[1, 8:12]], axis=0)
    f = fibers(azimuth, elevation)
    for i in range(3):
        fib[i, LAST : LAST + 8] = f[i]

    mine = slot[...]
    below = jnp.where(first_y, mine[0:1], srecv[0, 3:4])
    above = jnp.where(last_y, mine[3:4], srecv[1, 0:1])
    wanted = jnp.concatenate(
        [piece for row in (below, mine[0:1], mine[1:2], mine[2:3], mine[3:4], above) for piece in (row, row)],
        axis=1,
    )
    local = wanted & 255
    holder = (wanted >> 8) & (n_y - 1)
    from_o = (my_o - (holder >> (inner.bit_length() - 1))) & (outer - 1)
    from_i = (my_i - (holder & (inner - 1))) & (inner - 1)
    source = from_o * inner + from_i
    hot = jnp.where(
        lax.broadcasted_iota(jnp.int32, (256, 768), 0) == local, 1.0, 0.0
    ).astype(BF16)

    for copy in gathers:
        copy.wait_recv()
    d8 = ag8[...].reshape(n_y * 8, 256)
    d1 = ag1[...].reshape(n_y, 256)
    both = jnp.concatenate([d8, d1], axis=0)
    high = both.astype(BF16)
    low = (both - high.astype(F32)).astype(BF16)
    chosen = jnp.dot(high, hot, preferred_element_type=F32) + jnp.dot(
        low, hot, preferred_element_type=F32
    )
    total = jnp.zeros((8, 768), F32)
    for number in range(n_y):
        total = total + jnp.where(source == number, chosen[8 * number : 8 * number + 8], 0.0)
    s8[0] = total
    last = chosen[8 * n_y : 9 * n_y]
    s1[0] = jnp.sum(
        jnp.where(lax.broadcasted_iota(jnp.int32, (n_y, 768), 0) == source, last, 0.0),
        axis=0, keepdims=True,
    )
    for i in range(2):
        for (there, _, _), copies in zip(x_sides, coarse):
            send(there, copies[i : i + 1])

    for side, (there, _, x) in enumerate(x_sides):

        def own_plane(side=side, x=x):
            xpot[side] = pot[x]
            xang[side] = ang[:, x]
            for which in range(2):
                for i in (0, 3):
                    xcor[side, which, i : i + 1] = yrecv[which, x : x + 1]

        arrived(there, planes[1 - side] + corners[1 - side], own_plane)
    for side, start in ((0, 0), (1, 80)):
        f = fibers(xang[side, 0], xang[side, 1])
        for i in range(3):
            fib[i, start : start + 16] = f[i]
    volt = [xpot[0]] + [pot[x] for x in range(4)] + [xpot[1]]
    for which, row, outside in ((0, 0, first_y), (1, 15, last_y)):
        ring = [
            xcor[0, which, 3:4],
            yrecv[which, 0:1], yrecv[which, 1:2], yrecv[which, 2:3], yrecv[which, 3:4],
            xcor[1, which, 0:1],
        ]
        for p in range(6):
            vh[which, p : p + 1] = jnp.where(outside, volt[p][row : row + 1], ring[p])

    for copy in gathers:
        copy.wait_send()
    for (there, _, _), copies in zip(y_sides, halos):
        sent(there, copies)
    for (there, _, _), first, second in zip(x_sides, planes, corners):
        sent(there, first + second)

    for side, (there, _, _) in enumerate(x_sides):

        def own_elements(side=side):
            s8[1 + side] = s8[0]
            s1[1 + side] = s1[0]

        arrived(there, coarse[1 - side], own_elements)
    sub = lax.broadcasted_iota(jnp.int32, (8, 128), 0)

    def hat_rows(start, element):
        t = (sub.astype(F32) + (start + 0.5)) * 0.25 - 0.5
        return jnp.maximum(1.0 - jnp.abs(t - element), 0.0)

    tile0 = [hat_rows(0, e - 1) for e in range(4)]
    tile1 = [hat_rows(8, e + 1) for e in range(4)]
    t = ((sub & 3).astype(F32) + 0.5) * 0.25 - 0.5
    cross = [jnp.maximum(1.0 - jnp.abs(t - (e - 1)), 0.0) for e in range(3)]
    low_half = sub < 4
    for k in range(9):
        tiles0, tiles1, beside = [], [], []
        for which in (1, 0, 2):
            rows = []
            for e in range(6):
                lanes = slice(128 * e, 128 * e + 128)
                row = s8[which, k : k + 1, lanes] if k < 8 else s1[which, :, lanes]
                rows.append(jnp.broadcast_to(row, (8, 128)))
            tiles0.append(sum(tile0[i] * rows[i] for i in range(4)))
            tiles1.append(sum(tile1[i] * rows[i + 2] for i in range(4)))
            beside.append(
                jnp.where(low_half, 0.625 * rows[0] + 0.375 * rows[1], 0.625 * rows[5] + 0.375 * rows[4])
            )
        base = ROWS * k
        for p, (a, b, c) in enumerate(
            (
                (0.625, 0.375, 0.0), (0.375, 0.625, 0.0), (0.125, 0.875, 0.0),
                (0.0, 0.875, 0.125), (0.0, 0.625, 0.375), (0.0, 0.375, 0.625),
            )
        ):
            for half, tiles in ((0, tiles0), (8, tiles1)):
                if c == 0.0:
                    value = a * tiles[0] + b * tiles[1]
                else:
                    value = b * tiles[1] + c * tiles[2]
                crs[base + 16 * p + half : base + 16 * p + half + 8] = value
        crs[base + LAST : base + LAST + 8] = (
            cross[0] * beside[0] + cross[1] * beside[1] + cross[2] * beside[2]
        )
    c = crs[...]
    rest = c - c.astype(BF16).astype(F32)
    left = lax.broadcasted_iota(jnp.int32, c.shape, 1) < 64
    fine[...] = jnp.dot(
        jnp.where(left, c, rest).astype(BF16), hat, preferred_element_type=F32
    )

    for tile in range(13):
        at = 8 * tile
        f = [fine[ROWS * k + at : ROWS * k + at + 8] for k in range(9)]
        fiber = [fib[i, at : at + 8] for i in range(3)]
        own = 2 <= tile < 10
        d, s = tensor_rows(f, fiber, own)
        for i in range(6):
            con[i, at : at + 8] = d[i]
        if own:
            stretch[at - 16 : at - 8] = s

    row_iota = lax.broadcasted_iota(jnp.int32, (16, 256), 0)
    lane = lax.broadcasted_iota(jnp.int32, (16, 256), 1)

    def from_below(a, edge):
        return jnp.where(row_iota == 0, edge, pltpu.roll(a, 1, 0))

    def from_above(a, edge):
        return jnp.where(row_iota == 15, edge, pltpu.roll(a, 15, 0))

    def z_slope(v):
        n = v.shape[0]
        at = lax.broadcasted_iota(jnp.int32, (n, 256), 1)
        after = jnp.where(at == 255, v, pltpu.roll(v, 255, 1))
        before = jnp.where(at == 0, v, pltpu.roll(v, 1, 1))
        return after - before

    def flux(d1, step, d2, s2, d3, s3):
        return 0.5 * (d1 * step + 0.25 * (d2 * s2 + d3 * s3))

    XX, YY, ZZ, XY, XZ, YZ = range(6)
    slope_y = [from_above(volt[p], vh[1, p : p + 1]) - from_below(volt[p], vh[0, p : p + 1]) for p in range(6)]
    slope_z = [z_slope(volt[p]) for p in range(6)]
    edge_z = [z_slope(vh[which]) for which in range(2)]

    def plane(i, p):
        return con[i, 16 * p : 16 * p + 16]

    flux_x = []
    for p in range(5):
        value = flux(
            plane(XX, p) + plane(XX, p + 1), volt[p + 1] - volt[p],
            plane(XY, p) + plane(XY, p + 1), slope_y[p] + slope_y[p + 1],
            plane(XZ, p) + plane(XZ, p + 1), slope_z[p] + slope_z[p + 1],
        )
        if p == 0:
            value = jnp.where(first_x, 0.0, value)
        if p == 4:
            value = jnp.where(last_x, 0.0, value)
        flux_x.append(value)
    for x in range(4):
        p = x + 1
        v = volt[p]
        slope_x = volt[p + 1] - volt[p - 1]
        d_xy, d_yy, d_yz = plane(XY, p), plane(YY, p), plane(YZ, p)
        faces = []
        for which, shift in ((0, from_below), (1, from_above)):
            row = LAST + 4 * which + x
            step = shift(v, vh[which, p : p + 1])
            step = v - step if which == 0 else step - v
            faces.append(
                flux(
                    d_yy + shift(d_yy, con[YY, row : row + 1]), step,
                    d_xy + shift(d_xy, con[XY, row : row + 1]),
                    slope_x + shift(slope_x, vh[which, p + 1 : p + 2] - vh[which, p - 1 : p]),
                    d_yz + shift(d_yz, con[YZ, row : row + 1]),
                    slope_z[p] + shift(slope_z[p], edge_z[which][p : p + 1]),
                )
            )
        faces[0] = jnp.where((row_iota == 0) & first_y, 0.0, faces[0])
        faces[1] = jnp.where((row_iota == 15) & last_y, 0.0, faces[1])

        def onward(a):
            return pltpu.roll(a, 255, 1)

        d_xz, d_zz = plane(XZ, p), plane(ZZ, p)
        upper = flux(
            d_zz + onward(d_zz), onward(v) - v,
            d_xz + onward(d_xz), slope_x + onward(slope_x),
            d_yz + onward(d_yz), slope_y[p] + onward(slope_y[p]),
        )
        upper = jnp.where(lane == 255, 0.0, upper)
        divergent = (
            flux_x[p] - flux_x[p - 1] + (faces[1] - faces[0]) + (upper - pltpu.roll(upper, 1, 1))
        )
        w = rec[x]
        current = excite_gain * v * (v - excite_level) * (v - 1.0) + v * w
        current = current + stretch_gain * jnp.maximum(stretch[16 * x : 16 * x + 16] - 1.0, 0.0) * (
            v - stretch_reversal
        )
        onev[x] = v + time_step * (divergent - current)
    pot_store = pltpu.make_async_copy(onev, pot_out, out_sem.at[1])
    pot_store.start()
    for (there, _, _), copies in zip(x_sides, coarse):
        sent(there, copies)
    rec_store.wait()
    pot_store.wait()


def make_local(n_x, n_y):
    split = (4, 4) if n_y == 16 else (n_y // 2, 2)
    outer, inner = split

    def reach(number):
        o, i = number // inner, number % inner
        return min(o, outer - o) + 2 * min(i, inner - i)

    order = sorted(range(1, n_y), key=lambda number: -reach(number))

    def local(potential, recovery, fiber_angles, deform, elem_slot):
        anywhere = pl.BlockSpec(memory_space=pl.ANY)
        cells = (4, 16, 256)
        dma = pltpu.SemaphoreType.DMA
        call = pl.pallas_call(
            lambda *refs: kernel(n_x, n_y, split, order, *refs),
            out_shape=(jax.ShapeDtypeStruct(cells, F32),) * 2,
            in_specs=[anywhere] * 5,
            out_specs=(anywhere, anywhere),
            scratch_shapes=[
                pltpu.VMEM(cells, F32),
                pltpu.VMEM(cells, F32),
                pltpu.VMEM((2,) + cells, F32),
                pltpu.VMEM((9, 256), F32),
                pltpu.VMEM((4, 64), jnp.int32),
                pltpu.VMEM((n_y, 8, 256), F32),
                pltpu.VMEM((n_y, 1, 256), F32),
                pltpu.VMEM((2, 16, 256), F32),
                pltpu.VMEM((2, 16, 256), F32),
                pltpu.VMEM((2, 4, 64), jnp.int32),
                pltpu.VMEM((2, 16, 256), F32),
                pltpu.VMEM((2, 2, 16, 256), F32),
                pltpu.VMEM((2, 2, 8, 256), F32),
                pltpu.VMEM((3, 8, 768), F32),
                pltpu.VMEM((3, 1, 768), F32),
                pltpu.VMEM((3, ROWS, 256), F32),
                pltpu.VMEM((9 * ROWS, 128), F32),
                pltpu.VMEM((9 * ROWS, 256), F32),
                pltpu.VMEM((6, ROWS, 256), F32),
                pltpu.VMEM((64, 256), F32),
                pltpu.VMEM((2, 8, 256), F32),
                pltpu.VMEM(cells, F32),
                pltpu.VMEM(cells, F32),
                dma((5,)),
                dma((2,)),
                dma((2, n_y)),
                dma((2, n_y)),
                dma((2, 2)),
                dma((2, 2)),
                dma((5, 2)),
                dma((5, 2)),
                dma((2, 2)),
                dma((2, 2)),
            ],
            compiler_params=pltpu.CompilerParams(collective_id=0, has_side_effects=True),
            name="step",
        )
        return call(potential, recovery, fiber_angles, deform, elem_slot.reshape(4, 64))

    return local


def solution(mesh):
    placed = (
        P("gx", "gy", None),
        P("gx", "gy", None),
        P(None, "gx", "gy", None),
        P(None, ("gx", "gy")),
        P("gx", "gy", None),
    )
    return jax.shard_map(
        make_local(mesh.shape["gx"], mesh.shape["gy"]),
        mesh=mesh,
        in_specs=placed,
        out_specs=(P("gx", "gy", None), P("gx", "gy", None)),
        check_vma=False,
    )
```

```python
import jax
import jax.numpy as jnp
from jax import lax
from jax.experimental import pallas as pl
from jax.experimental.pallas import tpu as pltpu
from jax.sharding import PartitionSpec as P

sigma_fiber = 1.0
sigma_cross = 0.3
time_step = 0.1
excite_gain = 8.0
excite_level = 0.15
stretch_gain = 10.0
stretch_reversal = 0.6
recover_rate = 0.5

MESH = pl.DeviceIdType.MESH
F32 = jnp.float32
BF16 = jnp.bfloat16

ROWS = 104
LAST = 96


def sin_cos(angle):
    half = 0.5 * angle
    sq = half * half
    s = -2.5052108e-08
    for c in (2.7557319e-06, -1.9841270e-04, 8.3333333e-03, -1.6666667e-01, 1.0):
        s = s * sq + c
    s = s * half
    c2 = 2.0876757e-09
    for c in (-2.7557319e-07, 2.4801587e-05, -1.3888889e-03, 4.1666667e-02, -0.5, 1.0):
        c2 = c2 * sq + c
    return 2.0 * s * c2, 1.0 - 2.0 * s * s


def fibers(azimuth, elevation):
    sin_a, cos_a = sin_cos(azimuth)
    sin_e, cos_e = sin_cos(elevation)
    return cos_a * cos_e, sin_a * cos_e, sin_e


def tensor_rows(f, fiber, want_stretch):
    def el(i, j):
        return f[3 * (i % 3) + j % 3]

    cof = [
        [el(i + 1, j + 1) * el(i + 2, j + 2) - el(i + 1, j + 2) * el(i + 2, j + 1) for j in range(3)]
        for i in range(3)
    ]
    det = el(0, 0) * cof[0][0] + el(0, 1) * cof[0][1] + el(0, 2) * cof[0][2]
    inv = 1.0 / det
    scale = inv * inv
    stretch = None
    if want_stretch:
        st = [el(i, 0) * fiber[0] + el(i, 1) * fiber[1] + el(i, 2) * fiber[2] for i in range(3)]
        stretch = jnp.sqrt(st[0] * st[0] + st[1] * st[1] + st[2] * st[2])
    pulled = [cof[0][i] * fiber[0] + cof[1][i] * fiber[1] + cof[2][i] * fiber[2] for i in range(3)]
    out = []
    for a, b in ((0, 0), (1, 1), (2, 2), (0, 1), (0, 2), (1, 2)):
        metric = cof[0][a] * cof[0][b] + cof[1][a] * cof[1][b] + cof[2][a] * cof[2][b]
        out.append(
            (sigma_cross * metric + (sigma_fiber - sigma_cross) * pulled[a] * pulled[b]) * scale
        )
    return out, stretch


def spread(pair):
    other = pltpu.roll(pair, 64, 1)
    left = lax.broadcasted_iota(jnp.int32, pair.shape, 1) < 64
    return jnp.where(left, pair, other), jnp.where(left, other, pair)


def kernel(
    n_x, n_y, split, order,
    pot_in, rec_in, ang_in, def_in, slot_in, onev, onew,
    pot, rec, ang, slot, dfm, ag8, ag1, ysend, yrecv, srecv, beside_x, cc, s8, s1,
    fib, crs, fine, con, stretch, vh,
    in_sem, g_send, g_recv, s_send, s_recv, h_send, h_recv, p_send, p_recv, c_send, c_recv,
):
    gx = lax.axis_index("gx")
    gy = lax.axis_index("gy")
    first_x, last_x, first_y, last_y = gx == 0, gx == n_x - 1, gy == 0, gy == n_y - 1
    x_sides = ((jnp.logical_not(first_x), (gx - 1, gy), 0), (jnp.logical_not(last_x), (gx + 1, gy), 3))
    y_sides = ((jnp.logical_not(first_y), (gx, gy - 1), 0), (jnp.logical_not(last_y), (gx, gy + 1), 15))
    outer, inner = split
    my_o, my_i = lax.div(gy, inner), lax.rem(gy, inner)

    def peer(number):
        step_o, step_i = number // inner, number % inner
        return lax.rem(my_o + step_o, outer) * inner + lax.rem(my_i + step_i, inner)

    loads = [
        pltpu.make_async_copy(src, dst, in_sem.at[i])
        for i, (src, dst) in enumerate(
            ((def_in, dfm), (slot_in, slot), (pot_in, pot), (ang_in, ang), (rec_in, rec))
        )
    ]
    loads[0].start()
    barrier = pltpu.get_barrier_semaphore()
    for number in order:
        pl.semaphore_signal(barrier, inc=1, device_id=(gx, peer(number)), device_id_type=MESH)
    count = n_y - 1
    for there, device, *_ in x_sides:

        @pl.when(there)
        def _(device=device):
            pl.semaphore_signal(barrier, inc=1, device_id=device, device_id_type=MESH)

        count += jnp.where(there, 1, 0)

    for load in loads[1:]:
        load.start()
    loads[0].wait()
    ag8[0] = dfm[0:8]
    ag1[0] = dfm[8:9]
    for load in loads[1:]:
        load.wait()
    for side, (_, _, row) in enumerate(y_sides):
        ysend[side, 0:4] = pot[:, row, :]
        ysend[side, 4:8] = ang[0, :, row, :]
        ysend[side, 8:12] = ang[1, :, row, :]
    pl.semaphore_wait(barrier, count)

    def remote(src, dst, send_sem, recv_sem, device):
        return pltpu.make_async_remote_copy(
            src_ref=src, dst_ref=dst, send_sem=send_sem, recv_sem=recv_sem,
            device_id=device, device_id_type=MESH,
        )

    def send(there, copies):
        @pl.when(there)
        def _():
            for copy in copies:
                copy.start()

    def whole(ref, semaphore):
        return pltpu.make_async_copy(ref, ref, semaphore)

    def arrived(there, ref, semaphore, otherwise):
        @pl.when(there)
        def _():
            whole(ref, semaphore).wait()

        @pl.when(jnp.logical_not(there))
        def _():
            otherwise()

    def sent(there, ref, semaphore):
        @pl.when(there)
        def _():
            whole(ref, semaphore).wait()

    gathers = [
        remote(ref.at[0], ref.at[number], g_send.at[i], g_recv.at[i], (gx, peer(number)))
        for number in order
        for i, ref in enumerate((ag8, ag1))
    ]
    slots, halos, planes, coarse = [], [], [], []
    for side, (_, device, _) in enumerate(y_sides):
        slots.append(remote(slot, srecv.at[1 - side], s_send.at[side], s_recv.at[1 - side], device))
        halos.append(remote(ysend.at[side], yrecv.at[1 - side], h_send.at[side], h_recv.at[1 - side], device))
    for side, (_, device, x) in enumerate(x_sides):
        planes.append(
            [
                remote(
                    pot.at[x] if i == 0 else ang.at[i - 1, x], beside_x.at[1 - side, i],
                    p_send.at[side], p_recv.at[1 - side], device,
                )
                for i in range(3)
            ]
        )
        coarse.append(remote(cc.at[0], cc.at[2 - side], c_send.at[side], c_recv.at[1 - side], device))
    for (there, _, _), copy in zip(y_sides, slots):
        send(there, [copy])
    for copy in gathers:
        copy.start()
    for (there, _, _), copy in zip(y_sides, halos):
        send(there, [copy])
    for (there, _, _), copies in zip(x_sides, planes):
        send(there, copies)

    for x in range(4):
        v, w = pot[x], rec[x]
        onew[x] = w + time_step * recover_rate * (
            -w - excite_gain * v * (v - excite_level - 1.0)
        )
        f = fibers(ang[0, x], ang[1, x])
        for i in range(3):
            fib[i, 16 * (x + 1) : 16 * (x + 2)] = f[i]

    k_iota = lax.broadcasted_iota(jnp.int32, (128, 256), 0) & 63
    z_iota = lax.broadcasted_iota(jnp.int32, (128, 256), 1)
    place = jnp.clip((z_iota.astype(F32) + 0.5) * 0.25 - 0.5, 0.0, 63.0)
    hat = jnp.maximum(1.0 - jnp.abs(place - k_iota.astype(F32)), 0.0).astype(BF16)

    for side, (there, _, _) in enumerate(y_sides):

        def own_slots(side=side):
            srecv[side] = slot[...]

        arrived(there, srecv.at[side], s_recv.at[side], own_slots)
    mine = slot[...]
    below = jnp.where(first_y, mine[0:1], srecv[0, 3:4])
    above = jnp.where(last_y, mine[3:4], srecv[1, 0:1])
    wanted = jnp.concatenate(
        [below, mine[0:1], mine[1:2], mine[2:3], mine[3:4], above], axis=1
    )
    local = wanted & 255
    holder = (wanted >> 8) & (n_y - 1)
    from_o = (my_o - (holder >> (inner.bit_length() - 1))) & (outer - 1)
    from_i = (my_i - (holder & (inner - 1))) & (inner - 1)
    source = from_o * inner + from_i
    hot = jnp.where(
        lax.broadcasted_iota(jnp.int32, (256, 384), 0) == local, 1.0, 0.0
    ).astype(BF16)

    whole(ag8.at[1:n_y], g_recv.at[0]).wait()
    whole(ag1.at[1:n_y], g_recv.at[1]).wait()
    both = jnp.concatenate([ag8[...].reshape(n_y * 8, 256), ag1[...].reshape(n_y, 256)], axis=0)
    high = both.astype(BF16)
    low = (both - high.astype(F32)).astype(BF16)
    chosen = jnp.dot(high, hot, preferred_element_type=F32) + jnp.dot(
        low, hot, preferred_element_type=F32
    )
    total = jnp.zeros((8, 384), F32)
    for number in range(n_y):
        total = total + jnp.where(source == number, chosen[8 * number : 8 * number + 8], 0.0)
    last = chosen[8 * n_y : 9 * n_y]
    cc[0, 0:8] = total
    cc[0, 8:9] = jnp.sum(
        jnp.where(lax.broadcasted_iota(jnp.int32, (n_y, 384), 0) == source, last, 0.0),
        axis=0, keepdims=True,
    )

    for side, (there, _, row) in enumerate(y_sides):

        def own_row(side=side):
            yrecv[side, 0:12] = ysend[side, 0:12]

        arrived(there, yrecv.at[side], h_recv.at[side], own_row)
    for side, (there, _, x) in enumerate(x_sides):
        row = 9 + 2 * side
        for which in range(2):
            cc[0, row + which : row + which + 1, 0:256] = yrecv[which, x : x + 1]
    for (there, _, _), copy in zip(x_sides, coarse):
        send(there, [copy])

    for side, (there, _, x) in enumerate(x_sides):

        def own_plane(side=side, x=x):
            beside_x[side, 0] = pot[x]
            beside_x[side, 1:3] = ang[:, x]

        arrived(there, beside_x.at[side], p_recv.at[side], own_plane)
    azimuth = jnp.concatenate([yrecv[0, 4:8], yrecv[1, 4:8]], axis=0)
    elevation = jnp.concatenate([yrecv[0, 8:12], yrecv[1, 8:12]], axis=0)
    f = fibers(azimuth, elevation)
    for i in range(3):
        fib[i, LAST : LAST + 8] = f[i]
    for side, start in ((0, 0), (1, 80)):
        f = fibers(beside_x[side, 1], beside_x[side, 2])
        for i in range(3):
            fib[i, start : start + 16] = f[i]
    volt = [beside_x[0, 0]] + [pot[x] for x in range(4)] + [beside_x[1, 0]]
    for side, (there, _, _) in enumerate(x_sides):

        def own_elements(side=side):
            cc[1 + side] = cc[0]
            for which in range(2):
                row = 11 - 2 * side + which
                cc[1 + side, row : row + 1] = cc[0, 9 + 2 * side + which : 10 + 2 * side + which]

        arrived(there, cc.at[1 + side], c_recv.at[side], own_elements)
    for which, row, outside in ((0, 0, first_y), (1, 15, last_y)):
        ring = [cc[1, 11 + which : 12 + which, 0:256]]
        ring += [yrecv[which, x : x + 1] for x in range(4)]
        ring += [cc[2, 9 + which : 10 + which, 0:256]]
        for p in range(6):
            vh[which, p : p + 1] = jnp.where(outside, volt[p][row : row + 1], ring[p])
    for which in range(3):
        for rows, to in ((slice(0, 8), s8), (slice(8, 9), s1)):
            for i in range(3):
                pair = spread(cc[which, rows, 128 * i : 128 * i + 128])
                for j in range(2):
                    to[which, :, 128 * (2 * i + j) : 128 * (2 * i + j + 1)] = pair[j]
    sub = lax.broadcasted_iota(jnp.int32, (8, 128), 0)

    def hat_rows(start, element):
        t = (sub.astype(F32) + (start + 0.5)) * 0.25 - 0.5
        return jnp.maximum(1.0 - jnp.abs(t - element), 0.0)

    tile0 = [hat_rows(0, e - 1) for e in range(4)]
    tile1 = [hat_rows(8, e + 1) for e in range(4)]
    t = ((sub & 3).astype(F32) + 0.5) * 0.25 - 0.5
    cross = [jnp.maximum(1.0 - jnp.abs(t - (e - 1)), 0.0) for e in range(3)]
    low_half = sub < 4
    for k in range(9):
        tiles0, tiles1, beside = [], [], []
        for which in (1, 0, 2):
            rows = []
            for e in range(6):
                lanes = slice(128 * e, 128 * e + 128)
                row = s8[which, k : k + 1, lanes] if k < 8 else s1[which, :, lanes]
                rows.append(jnp.broadcast_to(row, (8, 128)))
            tiles0.append(sum(tile0[i] * rows[i] for i in range(4)))
            tiles1.append(sum(tile1[i] * rows[i + 2] for i in range(4)))
            beside.append(
                jnp.where(low_half, 0.625 * rows[0] + 0.375 * rows[1], 0.625 * rows[5] + 0.375 * rows[4])
            )
        base = ROWS * k
        for p, (a, b, c) in enumerate(
            (
                (0.625, 0.375, 0.0), (0.375, 0.625, 0.0), (0.125, 0.875, 0.0),
                (0.0, 0.875, 0.125), (0.0, 0.625, 0.375), (0.0, 0.375, 0.625),
            )
        ):
            for half, tiles in ((0, tiles0), (8, tiles1)):
                if c == 0.0:
                    value = a * tiles[0] + b * tiles[1]
                else:
                    value = b * tiles[1] + c * tiles[2]
                crs[base + 16 * p + half : base + 16 * p + half + 8] = value
        crs[base + LAST : base + LAST + 8] = (
            cross[0] * beside[0] + cross[1] * beside[1] + cross[2] * beside[2]
        )
    c = crs[...]
    rest = c - c.astype(BF16).astype(F32)
    left = lax.broadcasted_iota(jnp.int32, c.shape, 1) < 64
    fine[...] = jnp.dot(
        jnp.where(left, c, rest).astype(BF16), hat, preferred_element_type=F32
    )

    for tile in range(13):
        at = 8 * tile
        f = [fine[ROWS * k + at : ROWS * k + at + 8] for k in range(9)]
        fiber = [fib[i, at : at + 8] for i in range(3)]
        own = 2 <= tile < 10
        d, s = tensor_rows(f, fiber, own)
        for i in range(6):
            con[i, at : at + 8] = d[i]
        if own:
            stretch[at - 16 : at - 8] = s

    row_iota = lax.broadcasted_iota(jnp.int32, (16, 256), 0)
    lane = lax.broadcasted_iota(jnp.int32, (16, 256), 1)

    def from_below(a, edge):
        return jnp.where(row_iota == 0, edge, pltpu.roll(a, 1, 0))

    def from_above(a, edge):
        return jnp.where(row_iota == 15, edge, pltpu.roll(a, 15, 0))

    def z_slope(v):
        n = v.shape[0]
        at = lax.broadcasted_iota(jnp.int32, (n, 256), 1)
        after = jnp.where(at == 255, v, pltpu.roll(v, 255, 1))
        before = jnp.where(at == 0, v, pltpu.roll(v, 1, 1))
        return after - before

    def flux(d1, step, d2, s2, d3, s3):
        return 0.5 * (d1 * step + 0.25 * (d2 * s2 + d3 * s3))

    XX, YY, ZZ, XY, XZ, YZ = range(6)
    slope_y = [from_above(volt[p], vh[1, p : p + 1]) - from_below(volt[p], vh[0, p : p + 1]) for p in range(6)]
    slope_z = [z_slope(volt[p]) for p in range(6)]
    edge_z = [z_slope(vh[which]) for which in range(2)]

    def plane(i, p):
        return con[i, 16 * p : 16 * p + 16]

    flux_x = []
    for p in range(5):
        value = flux(
            plane(XX, p) + plane(XX, p + 1), volt[p + 1] - volt[p],
            plane(XY, p) + plane(XY, p + 1), slope_y[p] + slope_y[p + 1],
            plane(XZ, p) + plane(XZ, p + 1), slope_z[p] + slope_z[p + 1],
        )
        if p == 0:
            value = jnp.where(first_x, 0.0, value)
        if p == 4:
            value = jnp.where(last_x, 0.0, value)
        flux_x.append(value)
    for x in range(4):
        p = x + 1
        v = volt[p]
        slope_x = volt[p + 1] - volt[p - 1]
        d_xy, d_yy, d_yz = plane(XY, p), plane(YY, p), plane(YZ, p)
        faces = []
        for which, shift in ((0, from_below), (1, from_above)):
            row = LAST + 4 * which + x
            step = shift(v, vh[which, p : p + 1])
            step = v - step if which == 0 else step - v
            faces.append(
                flux(
                    d_yy + shift(d_yy, con[YY, row : row + 1]), step,
                    d_xy + shift(d_xy, con[XY, row : row + 1]),
                    slope_x + shift(slope_x, vh[which, p + 1 : p + 2] - vh[which, p - 1 : p]),
                    d_yz + shift(d_yz, con[YZ, row : row + 1]),
                    slope_z[p] + shift(slope_z[p], edge_z[which][p : p + 1]),
                )
            )
        faces[0] = jnp.where((row_iota == 0) & first_y, 0.0, faces[0])
        faces[1] = jnp.where((row_iota == 15) & last_y, 0.0, faces[1])

        def onward(a):
            return pltpu.roll(a, 255, 1)

        d_xz, d_zz = plane(XZ, p), plane(ZZ, p)
        upper = flux(
            d_zz + onward(d_zz), onward(v) - v,
            d_xz + onward(d_xz), slope_x + onward(slope_x),
            d_yz + onward(d_yz), slope_y[p] + onward(slope_y[p]),
        )
        upper = jnp.where(lane == 255, 0.0, upper)
        divergent = (
            flux_x[p] - flux_x[p - 1] + (faces[1] - faces[0]) + (upper - pltpu.roll(upper, 1, 1))
        )
        w = rec[x]
        current = excite_gain * v * (v - excite_level) * (v - 1.0) + v * w
        current = current + stretch_gain * jnp.maximum(stretch[16 * x : 16 * x + 16] - 1.0, 0.0) * (
            v - stretch_reversal
        )
        onev[x] = v + time_step * (divergent - current)
    whole(ag8.at[1:n_y], g_send.at[0]).wait()
    whole(ag1.at[1:n_y], g_send.at[1]).wait()
    for side, (there, _, _) in enumerate(y_sides):
        sent(there, srecv.at[side], s_send.at[side])
        sent(there, yrecv.at[side], h_send.at[side])
    for side, (there, _, _) in enumerate(x_sides):
        sent(there, beside_x.at[side], p_send.at[side])
        sent(there, cc.at[1 + side], c_send.at[side])


def store(pot, rec, pot_out, rec_out, sem):
    copies = [pltpu.make_async_copy(a, b, sem.at[i]) for i, (a, b) in enumerate(((pot, pot_out), (rec, rec_out)))]
    for copy in copies:
        copy.start()
    for copy in copies:
        copy.wait()


def make_local(n_x, n_y):
    split = (4, 4) if n_y == 16 else (n_y // 2, 2)
    outer, inner = split

    def reach(number):
        o, i = number // inner, number % inner
        return min(o, outer - o) + 2 * min(i, inner - i)

    order = sorted(range(1, n_y), key=lambda number: -reach(number))

    def local(potential, recovery, fiber_angles, deform, elem_slot):
        anywhere = pl.BlockSpec(memory_space=pl.ANY)
        cells = (4, 16, 256)
        dma = pltpu.SemaphoreType.DMA
        call = pl.pallas_call(
            lambda *refs: kernel(n_x, n_y, split, order, *refs),
            out_shape=(jax.ShapeDtypeStruct(cells, F32),) * 2,
            in_specs=[pl.BlockSpec(memory_space=pltpu.HBM)] * 5,
            out_specs=(pl.BlockSpec(memory_space=pltpu.VMEM),) * 2,
            scratch_shapes=[
                pltpu.VMEM(cells, F32),
                pltpu.VMEM(cells, F32),
                pltpu.VMEM((2,) + cells, F32),
                pltpu.VMEM((4, 64), jnp.int32),
                pltpu.VMEM((9, 256), F32),
                pltpu.VMEM((n_y, 8, 256), F32),
                pltpu.VMEM((n_y, 1, 256), F32),
                pltpu.VMEM((2, 16, 256), F32),
                pltpu.VMEM((2, 16, 256), F32),
                pltpu.VMEM((2, 4, 64), jnp.int32),
                pltpu.VMEM((2, 3, 16, 256), F32),
                pltpu.VMEM((3, 16, 384), F32),
                pltpu.VMEM((3, 8, 768), F32),
                pltpu.VMEM((3, 1, 768), F32),
                pltpu.VMEM((3, ROWS, 256), F32),
                pltpu.VMEM((9 * ROWS, 128), F32),
                pltpu.VMEM((9 * ROWS, 256), F32),
                pltpu.VMEM((6, ROWS, 256), F32),
                pltpu.VMEM((64, 256), F32),
                pltpu.VMEM((2, 8, 256), F32),
                dma((5,)),
                dma((2,)),
                dma((2,)),
                dma((2,)),
                dma((2,)),
                dma((2,)),
                dma((2,)),
                dma((2,)),
                dma((2,)),
                dma((2,)),
                dma((2,)),
            ],
            compiler_params=pltpu.CompilerParams(
                collective_id=0, has_side_effects=True, vmem_limit_bytes=16 * 2**20
            ),
            name="step",
        )
        args = (potential, recovery, fiber_angles, deform, elem_slot.reshape(4, 64))
        held = call(*(pltpu.with_memory_space_constraint(a, pltpu.HBM) for a in args))
        return pl.pallas_call(
            store,
            out_shape=(jax.ShapeDtypeStruct(cells, F32),) * 2,
            in_specs=[pl.BlockSpec(memory_space=pltpu.VMEM)] * 2,
            out_specs=(anywhere, anywhere),
            scratch_shapes=[dma((2,))],
            compiler_params=pltpu.CompilerParams(vmem_limit_bytes=16 * 2**20),
            name="store",
        )(*held)

    return local


def solution(mesh):
    placed = (
        P("gx", "gy", None),
        P("gx", "gy", None),
        P(None, "gx", "gy", None),
        P(None, ("gx", "gy")),
        P("gx", "gy", None),
    )
    return jax.shard_map(
        make_local(mesh.shape["gx"], mesh.shape["gy"]),
        mesh=mesh,
        in_specs=placed,
        out_specs=(P("gx", "gy", None), P("gx", "gy", None)),
        check_vma=False,
    )
```

```python
import jax
import jax.numpy as jnp
from jax import lax
from jax.experimental import pallas as pl
from jax.experimental.pallas import tpu as pltpu
from jax.sharding import PartitionSpec as P

sigma_fiber = 1.0
sigma_cross = 0.3
time_step = 0.1
excite_gain = 8.0
excite_level = 0.15
stretch_gain = 10.0
stretch_reversal = 0.6
recover_rate = 0.5

MESH = pl.DeviceIdType.MESH
F32 = jnp.float32
BF16 = jnp.bfloat16

HALF = 56
ROWS = 112


def plane_row(p):
    return 16 * p if p < 3 else HALF + 16 * (p - 3)


def beside_row(x, which):
    return 48 + HALF * (x // 2) + 2 * which + x % 2


def sin_cos(angle):
    half = 0.5 * angle
    sq = half * half
    s = -2.5052108e-08
    for c in (2.7557319e-06, -1.9841270e-04, 8.3333333e-03, -1.6666667e-01, 1.0):
        s = s * sq + c
    s = s * half
    c2 = 2.0876757e-09
    for c in (-2.7557319e-07, 2.4801587e-05, -1.3888889e-03, 4.1666667e-02, -0.5, 1.0):
        c2 = c2 * sq + c
    return 2.0 * s * c2, 1.0 - 2.0 * s * s


def fibers(azimuth, elevation):
    sin_a, cos_a = sin_cos(azimuth)
    sin_e, cos_e = sin_cos(elevation)
    return cos_a * cos_e, sin_a * cos_e, sin_e


def tensor_rows(f, fiber, want_stretch):
    def el(i, j):
        return f[3 * (i % 3) + j % 3]

    cof = [
        [el(i + 1, j + 1) * el(i + 2, j + 2) - el(i + 1, j + 2) * el(i + 2, j + 1) for j in range(3)]
        for i in range(3)
    ]
    det = el(0, 0) * cof[0][0] + el(0, 1) * cof[0][1] + el(0, 2) * cof[0][2]
    inv = 1.0 / det
    scale = inv * inv
    stretch = None
    if want_stretch:
        st = [el(i, 0) * fiber[0] + el(i, 1) * fiber[1] + el(i, 2) * fiber[2] for i in range(3)]
        stretch = jnp.sqrt(st[0] * st[0] + st[1] * st[1] + st[2] * st[2])
    pulled = [cof[0][i] * fiber[0] + cof[1][i] * fiber[1] + cof[2][i] * fiber[2] for i in range(3)]
    out = []
    for a, b in ((0, 0), (1, 1), (2, 2), (0, 1), (0, 2), (1, 2)):
        metric = cof[0][a] * cof[0][b] + cof[1][a] * cof[1][b] + cof[2][a] * cof[2][b]
        out.append(
            (sigma_cross * metric + (sigma_fiber - sigma_cross) * pulled[a] * pulled[b]) * scale
        )
    return out, stretch


def spread(pair):
    other = pltpu.roll(pair, 64, 1)
    left = lax.broadcasted_iota(jnp.int32, pair.shape, 1) < 64
    return jnp.where(left, pair, other), jnp.where(left, other, pair)


def kernel(
    n_x, n_y, split, order,
    pot_in, rec_in, ang_in, def_in, slot_in, onev, onew,
    pot, rec, ang, slot, dfm, ag8, ag1, ysend, yrecv, srecv, beside_x, cc, s8, s1,
    fib, mid, crs, fine, con, stretch, vh,
    in_sem, g_send, g_recv, s_send, s_recv, h_send, h_recv, p_send, p_recv, c_send, c_recv,
):
    gx = lax.axis_index("gx")
    gy = lax.axis_index("gy")
    first_x, last_x, first_y, last_y = gx == 0, gx == n_x - 1, gy == 0, gy == n_y - 1
    x_sides = ((jnp.logical_not(first_x), (gx - 1, gy), 0), (jnp.logical_not(last_x), (gx + 1, gy), 3))
    y_sides = ((jnp.logical_not(first_y), (gx, gy - 1), 0), (jnp.logical_not(last_y), (gx, gy + 1), 15))
    outer, inner = split
    my_o, my_i = lax.div(gy, inner), lax.rem(gy, inner)

    def peer(number):
        step_o, step_i = number // inner, number % inner
        return lax.rem(my_o + step_o, outer) * inner + lax.rem(my_i + step_i, inner)

    loads = [
        pltpu.make_async_copy(src, dst, in_sem.at[i])
        for i, (src, dst) in enumerate(
            ((def_in, dfm), (slot_in, slot), (pot_in, pot), (ang_in, ang), (rec_in, rec))
        )
    ]
    loads[0].start()
    barrier = pltpu.get_barrier_semaphore()
    for number in order:
        pl.semaphore_signal(barrier, inc=1, device_id=(gx, peer(number)), device_id_type=MESH)
    count = n_y - 1
    for there, device, *_ in x_sides:

        @pl.when(there)
        def _(device=device):
            pl.semaphore_signal(barrier, inc=1, device_id=device, device_id_type=MESH)

        count += jnp.where(there, 1, 0)

    for load in loads[1:]:
        load.start()
    loads[0].wait()
    ag8[0] = dfm[0:8]
    ag1[0] = dfm[8:9]
    for load in loads[1:]:
        load.wait()
    for side, (_, _, row) in enumerate(y_sides):
        ysend[side, 0:4] = pot[:, row, :]
        ysend[side, 4:8] = ang[0, :, row, :]
        ysend[side, 8:12] = ang[1, :, row, :]
    pl.semaphore_wait(barrier, count)

    def remote(src, dst, send_sem, recv_sem, device):
        return pltpu.make_async_remote_copy(
            src_ref=src, dst_ref=dst, send_sem=send_sem, recv_sem=recv_sem,
            device_id=device, device_id_type=MESH,
        )

    def send(there, copies):
        @pl.when(there)
        def _():
            for copy in copies:
                copy.start()

    def whole(ref, semaphore):
        return pltpu.make_async_copy(ref, ref, semaphore)

    def arrived(there, ref, semaphore, otherwise):
        @pl.when(there)
        def _():
            whole(ref, semaphore).wait()

        @pl.when(jnp.logical_not(there))
        def _():
            otherwise()

    def sent(there, ref, semaphore):
        @pl.when(there)
        def _():
            whole(ref, semaphore).wait()

    gathers = [
        remote(ref.at[0], ref.at[number], g_send.at[i], g_recv.at[i], (gx, peer(number)))
        for number in order
        for i, ref in enumerate((ag8, ag1))
    ]
    slots, halos, planes, coarse = [], [], [], []
    for side, (_, device, _) in enumerate(y_sides):
        slots.append(remote(slot, srecv.at[1 - side], s_send.at[side], s_recv.at[1 - side], device))
        halos.append(remote(ysend.at[side], yrecv.at[1 - side], h_send.at[side], h_recv.at[1 - side], device))
    for side, (_, device, x) in enumerate(x_sides):
        planes.append(
            [
                remote(
                    pot.at[x] if i == 0 else ang.at[i - 1, x], beside_x.at[1 - side, i],
                    p_send.at[side], p_recv.at[1 - side], device,
                )
                for i in range(3)
            ]
        )
        coarse.append(remote(cc.at[0], cc.at[2 - side], c_send.at[side], c_recv.at[1 - side], device))
    for (there, _, _), copy in zip(y_sides, slots):
        send(there, [copy])
    for copy in gathers:
        copy.start()
    for (there, _, _), copy in zip(y_sides, halos):
        send(there, [copy])
    for (there, _, _), copies in zip(x_sides, planes):
        send(there, copies)

    for x in range(4):
        v, w = pot[x], rec[x]
        onew[x] = w + time_step * recover_rate * (
            -w - excite_gain * v * (v - excite_level - 1.0)
        )
        f = fibers(ang[0, x], ang[1, x])
        for i in range(3):
            fib[i, plane_row(x + 1) : plane_row(x + 1) + 16] = f[i]

    k_iota = lax.broadcasted_iota(jnp.int32, (128, 256), 0) & 63
    z_iota = lax.broadcasted_iota(jnp.int32, (128, 256), 1)
    place = jnp.clip((z_iota.astype(F32) + 0.5) * 0.25 - 0.5, 0.0, 63.0)
    hat = jnp.maximum(1.0 - jnp.abs(place - k_iota.astype(F32)), 0.0).astype(BF16)

    for side, (there, _, _) in enumerate(y_sides):

        def own_slots(side=side):
            srecv[side] = slot[...]

        arrived(there, srecv.at[side], s_recv.at[side], own_slots)
    mine = slot[...]
    below = jnp.where(first_y, mine[0:1], srecv[0, 3:4])
    above = jnp.where(last_y, mine[3:4], srecv[1, 0:1])
    wanted = jnp.concatenate(
        [below, mine[0:1], mine[1:2], mine[2:3], mine[3:4], above], axis=1
    )
    local = wanted & 255
    holder = (wanted >> 8) & (n_y - 1)
    from_o = (my_o - (holder >> (inner.bit_length() - 1))) & (outer - 1)
    from_i = (my_i - (holder & (inner - 1))) & (inner - 1)
    source = from_o * inner + from_i
    hot = jnp.where(
        lax.broadcasted_iota(jnp.int32, (256, 384), 0) == local, 1.0, 0.0
    ).astype(BF16)

    whole(ag8.at[1:n_y], g_recv.at[0]).wait()
    whole(ag1.at[1:n_y], g_recv.at[1]).wait()
    both = jnp.concatenate([ag8[...].reshape(n_y * 8, 256), ag1[...].reshape(n_y, 256)], axis=0)
    high = both.astype(BF16)
    low = (both - high.astype(F32)).astype(BF16)
    chosen = jnp.dot(high, hot, preferred_element_type=F32) + jnp.dot(
        low, hot, preferred_element_type=F32
    )
    total = jnp.zeros((8, 384), F32)
    for number in range(n_y):
        total = total + jnp.where(source == number, chosen[8 * number : 8 * number + 8], 0.0)
    last = chosen[8 * n_y : 9 * n_y]
    cc[0, 0:8] = total
    cc[0, 8:9] = jnp.sum(
        jnp.where(lax.broadcasted_iota(jnp.int32, (n_y, 384), 0) == source, last, 0.0),
        axis=0, keepdims=True,
    )

    for side, (there, _, row) in enumerate(y_sides):

        def own_row(side=side):
            yrecv[side, 0:12] = ysend[side, 0:12]

        arrived(there, yrecv.at[side], h_recv.at[side], own_row)
    for side, (there, _, x) in enumerate(x_sides):
        row = 9 + 2 * side
        for which in range(2):
            cc[0, row + which : row + which + 1, 0:256] = yrecv[which, x : x + 1]
    for (there, _, _), copy in zip(x_sides, coarse):
        send(there, [copy])

    def onto_lanes(which):
        for rows, to in ((slice(0, 8), s8), (slice(8, 9), s1)):
            for i in range(3):
                pair = spread(cc[which, rows, 128 * i : 128 * i + 128])
                for j in range(2):
                    to[which, :, 128 * (2 * i + j) : 128 * (2 * i + j + 1)] = pair[j]

    sub = lax.broadcasted_iota(jnp.int32, (8, 128), 0)

    def hat_rows(at, element):
        t = at.astype(F32) * 0.25 + (0.125 - 0.5)
        return jnp.maximum(1.0 - jnp.abs(t - element), 0.0)

    tile0 = [hat_rows(sub, e - 1) for e in range(4)]
    tile1 = [hat_rows(sub + 8, e + 1) for e in range(4)]

    def along_y(which, k):
        rows = []
        for e in range(6):
            lanes = slice(128 * e, 128 * e + 128)
            row = s8[which, k : k + 1, lanes] if k < 8 else s1[which, :, lanes]
            rows.append(jnp.broadcast_to(row, (8, 128)))
        return (
            sum(tile0[i] * rows[i] for i in range(4)),
            sum(tile1[i] * rows[i + 2] for i in range(4)),
            jnp.where(
                (sub & 2) == 0, 0.625 * rows[0] + 0.375 * rows[1], 0.625 * rows[5] + 0.375 * rows[4]
            ),
        )

    onto_lanes(0)
    for k in range(9):
        for i, value in enumerate(along_y(0, k)):
            mid[k, i] = value
    for half in range(2):
        crs[half, 9 * HALF :] = jnp.zeros((8, 128), F32)
        rows = [yrecv[which, at + 2 * half : at + 2 * half + 2] for at in (4, 8) for which in range(2)]
        f = fibers(
            jnp.concatenate([rows[0], rows[1]] * 2, axis=0), jnp.concatenate([rows[2], rows[3]] * 2, axis=0)
        )
        for i in range(3):
            fib[i, HALF * half + 48 : HALF * half + 56] = f[i]
    row_iota = lax.broadcasted_iota(jnp.int32, (16, 256), 0)
    lane = lax.broadcasted_iota(jnp.int32, (16, 256), 1)

    def from_below(a, edge):
        return jnp.where(row_iota == 0, edge, pltpu.roll(a, 1, 0))

    def from_above(a, edge):
        return jnp.where(row_iota == 15, edge, pltpu.roll(a, 15, 0))

    def onward(a):
        return pltpu.roll(a, 255, 1)

    def z_slope(v):
        at = lax.broadcasted_iota(jnp.int32, v.shape, 1)
        after = jnp.where(at == 255, v, pltpu.roll(v, 255, 1))
        before = jnp.where(at == 0, v, pltpu.roll(v, 1, 1))
        return after - before

    def flux(d1, step, d2, s2, d3, s3):
        return 0.5 * (d1 * step + 0.25 * (d2 * s2 + d3 * s3))

    XX, YY, ZZ, XY, XZ, YZ = range(6)

    def plane(i, p):
        return con[i, plane_row(p) : plane_row(p) + 16]

    ends = ((0, 0, first_y), (1, 15, last_y))
    for which, row, outside in ends:
        vh[which] = jnp.zeros((8, 256), F32)
        for x in range(4):
            vh[which, x + 1 : x + 2] = jnp.where(outside, pot[x, row : row + 1], yrecv[which, x : x + 1])

    slope_y, slope_z = [None] * 6, [None] * 6
    between = None
    for half, (there, _, x) in enumerate(x_sides):

        def own_plane(half=half, x=x):
            beside_x[half, 0] = pot[x]
            beside_x[half, 1:3] = ang[:, x]

        def own_elements(half=half):
            cc[1 + half] = cc[0]
            for which in range(2):
                row = 11 - 2 * half + which
                cc[1 + half, row : row + 1] = cc[0, 9 + 2 * half + which : 10 + 2 * half + which]

        arrived(there, beside_x.at[half], p_recv.at[half], own_plane)
        f = fibers(beside_x[half, 1], beside_x[half, 2])
        outer_p = 5 * half
        for i in range(3):
            fib[i, plane_row(outer_p) : plane_row(outer_p) + 16] = f[i]
        arrived(there, cc.at[1 + half], c_recv.at[half], own_elements)

        onto_lanes(1 + half)
        t = hat_rows((sub & 1) + 2 * half, 0), hat_rows((sub & 1) + 2 * half, 2 * half - 1)
        weights = ((0.625, 0.375), (0.375, 0.625), (0.125, 0.875))
        for k in range(9):
            side = along_y(1 + half, k)
            base = HALF * k
            for number, (a, b) in enumerate(weights[:: 1 - 2 * half]):
                for i in range(2):
                    at = base + 16 * number + 8 * i
                    crs[half, at : at + 8] = a * side[i] + b * mid[k, i]
            crs[half, base + 48 : base + 56] = t[0] * mid[k, 2] + t[1] * side[2]
        c = crs[half]
        rest = c - c.astype(BF16).astype(F32)
        left = lax.broadcasted_iota(jnp.int32, c.shape, 1) < 64
        fine[half] = jnp.dot(
            jnp.where(left, c, rest).astype(BF16), hat, preferred_element_type=F32
        )
        for tile in range(7):
            at = 8 * tile
            row = HALF * half + at
            f = [fine[half, HALF * k + at : HALF * k + at + 8] for k in range(9)]
            fiber = [fib[i, row : row + 8] for i in range(3)]
            inside = (2 <= tile < 6) if half == 0 else tile < 4
            d, length = tensor_rows(f, fiber, inside)
            for i in range(6):
                con[i, row : row + 8] = d[i]
            if inside:
                stretch[row : row + 8] = length

        for which, row, outside in ends:
            corner = cc[1 + half, 11 - 2 * half + which : 12 - 2 * half + which, 0:256]
            vh[which, outer_p : outer_p + 1] = jnp.where(outside, beside_x[half, 0, row : row + 1], corner)
        volt = [beside_x[0, 0]] + [pot[x] for x in range(4)] + [beside_x[1, 0]]
        edge_z = [z_slope(vh[which]) for which in range(2)]
        for p in range(3 * half, 3 * half + 3):
            slope_y[p] = from_above(volt[p], vh[1, p : p + 1]) - from_below(volt[p], vh[0, p : p + 1])
            slope_z[p] = z_slope(volt[p])

        def across(p):
            return flux(
                plane(XX, p) + plane(XX, p + 1), volt[p + 1] - volt[p],
                plane(XY, p) + plane(XY, p + 1), slope_y[p] + slope_y[p + 1],
                plane(XZ, p) + plane(XZ, p + 1), slope_z[p] + slope_z[p + 1],
            )

        def within(x):
            p = x + 1
            v = volt[p]
            slope_x = volt[p + 1] - volt[p - 1]
            d_xy, d_yy, d_yz = plane(XY, p), plane(YY, p), plane(YZ, p)
            faces = []
            for which, shift in ((0, from_below), (1, from_above)):
                row = beside_row(x, which)
                step = shift(v, vh[which, p : p + 1])
                step = v - step if which == 0 else step - v
                faces.append(
                    flux(
                        d_yy + shift(d_yy, con[YY, row : row + 1]), step,
                        d_xy + shift(d_xy, con[XY, row : row + 1]),
                        slope_x + shift(slope_x, vh[which, p + 1 : p + 2] - vh[which, p - 1 : p]),
                        d_yz + shift(d_yz, con[YZ, row : row + 1]),
                        slope_z[p] + shift(slope_z[p], edge_z[which][p : p + 1]),
                    )
                )
            faces[0] = jnp.where((row_iota == 0) & first_y, 0.0, faces[0])
            faces[1] = jnp.where((row_iota == 15) & last_y, 0.0, faces[1])
            d_xz, d_zz = plane(XZ, p), plane(ZZ, p)
            upper = flux(
                d_zz + onward(d_zz), onward(v) - v,
                d_xz + onward(d_xz), slope_x + onward(slope_x),
                d_yz + onward(d_yz), slope_y[p] + onward(slope_y[p]),
            )
            upper = jnp.where(lane == 255, 0.0, upper)
            w = rec[x]
            current = excite_gain * v * (v - excite_level) * (v - 1.0) + v * w
            long = jnp.maximum(stretch[plane_row(p) : plane_row(p) + 16] - 1.0, 0.0)
            current = current + stretch_gain * long * (v - stretch_reversal)
            divergent = (faces[1] - faces[0]) + (upper - pltpu.roll(upper, 1, 1))
            return v + time_step * (divergent - current)

        if half == 0:
            below = jnp.where(first_x, 0.0, across(0))
            middle = across(1)
            onev[0] = within(0) + time_step * (middle - below)
            onev[1] = within(1) - time_step * middle
        else:
            middle = across(2)
            upper_face = across(3)
            last_face = jnp.where(last_x, 0.0, across(4))
            onev[1] = onev[1] + time_step * middle
            onev[2] = within(2) + time_step * (upper_face - middle)
            onev[3] = within(3) + time_step * (last_face - upper_face)
    whole(ag8.at[1:n_y], g_send.at[0]).wait()
    whole(ag1.at[1:n_y], g_send.at[1]).wait()
    for side, (there, _, _) in enumerate(y_sides):
        sent(there, srecv.at[side], s_send.at[side])
        sent(there, yrecv.at[side], h_send.at[side])
    for side, (there, _, _) in enumerate(x_sides):
        sent(there, beside_x.at[side], p_send.at[side])
        sent(there, cc.at[1 + side], c_send.at[side])


def store(pot, rec, pot_out, rec_out, sem):
    copies = [pltpu.make_async_copy(a, b, sem.at[i]) for i, (a, b) in enumerate(((pot, pot_out), (rec, rec_out)))]
    for copy in copies:
        copy.start()
    for copy in copies:
        copy.wait()


def make_local(n_x, n_y):
    split = (4, 4) if n_y == 16 else (n_y // 2, 2)
    outer, inner = split

    def reach(number):
        o, i = number // inner, number % inner
        return min(o, outer - o) + 2 * min(i, inner - i)

    order = sorted(range(1, n_y), key=lambda number: -reach(number))

    def local(potential, recovery, fiber_angles, deform, elem_slot):
        anywhere = pl.BlockSpec(memory_space=pl.ANY)
        cells = (4, 16, 256)
        dma = pltpu.SemaphoreType.DMA
        call = pl.pallas_call(
            lambda *refs: kernel(n_x, n_y, split, order, *refs),
            out_shape=(jax.ShapeDtypeStruct(cells, F32),) * 2,
            in_specs=[pl.BlockSpec(memory_space=pltpu.HBM)] * 5,
            out_specs=(pl.BlockSpec(memory_space=pltpu.VMEM),) * 2,
            scratch_shapes=[
                pltpu.VMEM(cells, F32),
                pltpu.VMEM(cells, F32),
                pltpu.VMEM((2,) + cells, F32),
                pltpu.VMEM((4, 64), jnp.int32),
                pltpu.VMEM((9, 256), F32),
                pltpu.VMEM((n_y, 8, 256), F32),
                pltpu.VMEM((n_y, 1, 256), F32),
                pltpu.VMEM((2, 16, 256), F32),
                pltpu.VMEM((2, 16, 256), F32),
                pltpu.VMEM((2, 4, 64), jnp.int32),
                pltpu.VMEM((2, 3, 16, 256), F32),
                pltpu.VMEM((3, 16, 384), F32),
                pltpu.VMEM((3, 8, 768), F32),
                pltpu.VMEM((3, 1, 768), F32),
                pltpu.VMEM((3, ROWS, 256), F32),
                pltpu.VMEM((9, 3, 8, 128), F32),
                pltpu.VMEM((2, 9 * HALF + 8, 128), F32),
                pltpu.VMEM((2, 9 * HALF + 8, 256), F32),
                pltpu.VMEM((6, ROWS, 256), F32),
                pltpu.VMEM((ROWS, 256), F32),
                pltpu.VMEM((2, 8, 256), F32),
                dma((5,)),
                dma((2,)),
                dma((2,)),
                dma((2,)),
                dma((2,)),
                dma((2,)),
                dma((2,)),
                dma((2,)),
                dma((2,)),
                dma((2,)),
                dma((2,)),
            ],
            compiler_params=pltpu.CompilerParams(
                collective_id=0, has_side_effects=True, vmem_limit_bytes=16 * 2**20
            ),
            name="step",
        )
        args = (potential, recovery, fiber_angles, deform, elem_slot.reshape(4, 64))
        held = call(*(pltpu.with_memory_space_constraint(a, pltpu.HBM) for a in args))
        return pl.pallas_call(
            store,
            out_shape=(jax.ShapeDtypeStruct(cells, F32),) * 2,
            in_specs=[pl.BlockSpec(memory_space=pltpu.VMEM)] * 2,
            out_specs=(anywhere, anywhere),
            scratch_shapes=[dma((2,))],
            compiler_params=pltpu.CompilerParams(vmem_limit_bytes=16 * 2**20),
            name="store",
        )(*held)

    return local


def solution(mesh):
    placed = (
        P("gx", "gy", None),
        P("gx", "gy", None),
        P(None, "gx", "gy", None),
        P(None, ("gx", "gy")),
        P("gx", "gy", None),
    )
    return jax.shard_map(
        make_local(mesh.shape["gx"], mesh.shape["gy"]),
        mesh=mesh,
        in_specs=placed,
        out_specs=(P("gx", "gy", None), P("gx", "gy", None)),
        check_vma=False,
    )
```

```python
import jax
import jax.numpy as jnp
from jax import lax
from jax.experimental import pallas as pl
from jax.experimental.pallas import tpu as pltpu
from jax.sharding import PartitionSpec as P

sigma_fiber = 1.0
sigma_cross = 0.3
time_step = 0.1
excite_gain = 8.0
excite_level = 0.15
stretch_gain = 10.0
stretch_reversal = 0.6
recover_rate = 0.5

MESH = pl.DeviceIdType.MESH
F32 = jnp.float32
BF16 = jnp.bfloat16

HALF = 56
ROWS = 112


def plane_row(p):
    return 16 * p if p < 3 else HALF + 16 * (p - 3)


def beside_row(x, which):
    return 48 + HALF * (x // 2) + 2 * which + x % 2


def sin_cos(angle):
    half = 0.5 * angle
    sq = half * half
    s = -2.5052108e-08
    for c in (2.7557319e-06, -1.9841270e-04, 8.3333333e-03, -1.6666667e-01, 1.0):
        s = s * sq + c
    s = s * half
    c2 = 2.0876757e-09
    for c in (-2.7557319e-07, 2.4801587e-05, -1.3888889e-03, 4.1666667e-02, -0.5, 1.0):
        c2 = c2 * sq + c
    return 2.0 * s * c2, 1.0 - 2.0 * s * s


def fibers(azimuth, elevation):
    sin_a, cos_a = sin_cos(azimuth)
    sin_e, cos_e = sin_cos(elevation)
    return cos_a * cos_e, sin_a * cos_e, sin_e


def tensor_rows(f, fiber, want_stretch):
    def el(i, j):
        return f[3 * (i % 3) + j % 3]

    cof = [
        [el(i + 1, j + 1) * el(i + 2, j + 2) - el(i + 1, j + 2) * el(i + 2, j + 1) for j in range(3)]
        for i in range(3)
    ]
    det = el(0, 0) * cof[0][0] + el(0, 1) * cof[0][1] + el(0, 2) * cof[0][2]
    inv = 1.0 / det
    scale = inv * inv
    stretch = None
    if want_stretch:
        st = [el(i, 0) * fiber[0] + el(i, 1) * fiber[1] + el(i, 2) * fiber[2] for i in range(3)]
        stretch = jnp.sqrt(st[0] * st[0] + st[1] * st[1] + st[2] * st[2])
    pulled = [cof[0][i] * fiber[0] + cof[1][i] * fiber[1] + cof[2][i] * fiber[2] for i in range(3)]
    out = []
    for a, b in ((0, 0), (1, 1), (2, 2), (0, 1), (0, 2), (1, 2)):
        metric = cof[0][a] * cof[0][b] + cof[1][a] * cof[1][b] + cof[2][a] * cof[2][b]
        out.append(
            (sigma_cross * metric + (sigma_fiber - sigma_cross) * pulled[a] * pulled[b]) * scale
        )
    return out, stretch


STRAIGHT = ((1, 0), (2, 0), (3, 0), (1, 1), (1, 3), (3, 1), (3, 3))
COLUMN = ((0, 1), (0, 3), (0, 2))
RELAYED = ((2, 1), (2, 3), (1, 2), (2, 2), (3, 2))
PLACES = ((0, 0),) + STRAIGHT + COLUMN + RELAYED


def spread(pair):
    other = pltpu.roll(pair, 64, 1)
    left = lax.broadcasted_iota(jnp.int32, pair.shape, 1) < 64
    return jnp.where(left, pair, other), jnp.where(left, other, pair)


def kernel(
    n_x, n_y,
    pot_in, rec_in, ang_in, def_in, slot_in, onev, onew,
    pot, rec, ang, slot, dfm, ag8, ag1, ysend, yrecv, srecv, beside_x, cc, s8, s1,
    fib, mid, crs, fine, con, stretch, vh,
    in_sem, g_send, g_recv, s_send, s_recv, h_send, h_recv, p_send, p_recv, c_send, c_recv,
):
    gx = lax.axis_index("gx")
    gy = lax.axis_index("gy")
    first_x, last_x, first_y, last_y = gx == 0, gx == n_x - 1, gy == 0, gy == n_y - 1
    x_sides = ((jnp.logical_not(first_x), (gx - 1, gy), 0), (jnp.logical_not(last_x), (gx + 1, gy), 3))
    y_sides = ((jnp.logical_not(first_y), (gx, gy - 1), 0), (jnp.logical_not(last_y), (gx, gy + 1), 15))
    my_o, my_i = lax.div(gy, 4), lax.rem(gy, 4)

    def peer(o, i):
        return (gx, lax.rem(my_o + o, 4) * 4 + lax.rem(my_i + i, 4))

    direct = ((0, 2), (0, 1), (0, 3), (1, 1), (1, 3), (3, 1), (3, 3), (2, 0), (1, 0), (3, 0))
    every = (
        (2, 2), (1, 2), (3, 2), (0, 2), (2, 1), (2, 3), (1, 1), (1, 3), (3, 1), (3, 3),
        (0, 1), (0, 3), (2, 0), (1, 0), (3, 0),
    )
    late = lax.rem(gx, 2) == 0

    loads = [
        pltpu.make_async_copy(src, dst, in_sem.at[i])
        for i, (src, dst) in enumerate(
            ((def_in, dfm), (slot_in, slot), (pot_in, pot), (ang_in, ang), (rec_in, rec))
        )
    ]
    loads[0].start()
    barrier = pltpu.get_barrier_semaphore()
    for steps in direct:
        pl.semaphore_signal(barrier, inc=1, device_id=peer(*steps), device_id_type=MESH)

    @pl.when(late)
    def _():
        for steps in RELAYED:
            pl.semaphore_signal(barrier, inc=1, device_id=peer(*steps), device_id_type=MESH)

    count = len(direct) + jnp.where(late, len(RELAYED), 0)
    for there, device, *_ in x_sides:

        @pl.when(there)
        def _(device=device):
            pl.semaphore_signal(barrier, inc=1, device_id=device, device_id_type=MESH)

        count += jnp.where(there, 1, 0)

    for load in loads[1:]:
        load.start()
    loads[0].wait()
    ag8[0] = dfm[0:8]
    ag1[0] = dfm[8:9]
    for load in loads[1:]:
        load.wait()
    for side, (_, _, row) in enumerate(y_sides):
        ysend[side, 0:4] = pot[:, row, :]
        ysend[side, 4:8] = ang[0, :, row, :]
        ysend[side, 8:12] = ang[1, :, row, :]
    pl.semaphore_wait(barrier, count)

    def remote(src, dst, send_sem, recv_sem, device):
        return pltpu.make_async_remote_copy(
            src_ref=src, dst_ref=dst, send_sem=send_sem, recv_sem=recv_sem,
            device_id=device, device_id_type=MESH,
        )

    def send(there, copies):
        @pl.when(there)
        def _():
            for copy in copies:
                copy.start()

    def whole(ref, semaphore):
        return pltpu.make_async_copy(ref, ref, semaphore)

    def arrived(there, ref, semaphore, otherwise):
        @pl.when(there)
        def _():
            whole(ref, semaphore).wait()

        @pl.when(jnp.logical_not(there))
        def _():
            otherwise()

    def sent(there, ref, semaphore):
        @pl.when(there)
        def _():
            whole(ref, semaphore).wait()

    def piece(place, steps, device, group):
        return [
            remote(ref.at[place], ref.at[PLACES.index(steps)], g_send.at[k], g_recv.at[group, k], device)
            for k, ref in enumerate((ag8, ag1))
        ]

    def gather(steps):
        group = 1 + COLUMN.index(steps) if steps in COLUMN else 4 if steps in RELAYED else 0
        for copy in piece(0, steps, peer(*steps), group):
            copy.start()

    def relay(steps):
        at, group = PLACES.index(steps), 1 + COLUMN.index(steps)
        for k, ref in enumerate((ag8, ag1)):
            whole(ref.at[at], g_recv.at[group, k]).wait()

        @pl.when(jnp.logical_not(late))
        def _():
            for o in (2, 1, 3):
                to = (o, steps[1])
                for copy in piece(at, to, peer(o, 0), 4 if to in RELAYED else 0):
                    copy.start()

    slots, halos, planes, coarse = [], [], [], []
    for side, (_, device, _) in enumerate(y_sides):
        slots.append(remote(slot, srecv.at[1 - side], s_send.at[side], s_recv.at[1 - side], device))
        halos.append(remote(ysend.at[side], yrecv.at[1 - side], h_send.at[side], h_recv.at[1 - side], device))
    for side, (_, device, x) in enumerate(x_sides):
        planes.append(
            [
                remote(
                    pot.at[x] if i == 0 else ang.at[i - 1, x], beside_x.at[1 - side, i],
                    p_send.at[side], p_recv.at[1 - side], device,
                )
                for i in range(3)
            ]
        )
        coarse.append(remote(cc.at[0], cc.at[2 - side], c_send.at[side], c_recv.at[1 - side], device))
    for (there, _, _), copy in zip(y_sides, slots):
        send(there, [copy])

    @pl.when(late)
    def _():
        for steps in every:
            gather(steps)

    @pl.when(jnp.logical_not(late))
    def _():
        for steps in direct:
            if 0 in steps:
                gather(steps)

    for (there, _, _), copy in zip(y_sides, halos):
        send(there, [copy])
    for (there, _, _), copies in zip(x_sides, planes):
        send(there, copies)

    for x in range(4):
        v, w = pot[x], rec[x]
        onew[x] = w + time_step * recover_rate * (
            -w - excite_gain * v * (v - excite_level - 1.0)
        )
        f = fibers(ang[0, x], ang[1, x])
        for i in range(3):
            fib[i, plane_row(x + 1) : plane_row(x + 1) + 16] = f[i]

    k_iota = lax.broadcasted_iota(jnp.int32, (128, 256), 0) & 63
    z_iota = lax.broadcasted_iota(jnp.int32, (128, 256), 1)
    place = jnp.clip((z_iota.astype(F32) + 0.5) * 0.25 - 0.5, 0.0, 63.0)
    hat = jnp.maximum(1.0 - jnp.abs(place - k_iota.astype(F32)), 0.0).astype(BF16)

    relay((0, 1))
    relay((0, 3))

    for side, (there, _, _) in enumerate(y_sides):

        def own_slots(side=side):
            srecv[side] = slot[...]

        arrived(there, srecv.at[side], s_recv.at[side], own_slots)
    mine = slot[...]
    below = jnp.where(first_y, mine[0:1], srecv[0, 3:4])
    above = jnp.where(last_y, mine[3:4], srecv[1, 0:1])
    wanted = jnp.concatenate(
        [below, mine[0:1], mine[1:2], mine[2:3], mine[3:4], above], axis=1
    )
    local = wanted & 255
    source = (((my_o - (wanted >> 10)) & 3) << 2) | ((my_i - (wanted >> 8)) & 3)
    place_iota = lax.broadcasted_iota(jnp.int32, (n_y, 384), 0)
    place_source = sum(jnp.where(place_iota == at, 4 * o + i, 0) for at, (o, i) in enumerate(PLACES))
    hot = jnp.where(
        lax.broadcasted_iota(jnp.int32, (256, 384), 0) == local, 1.0, 0.0
    ).astype(BF16)

    relay((0, 2))

    for k, ref in enumerate((ag8, ag1)):
        whole(ref.at[1:8], g_recv.at[0, k]).wait()
        whole(ref.at[11:16], g_recv.at[4, k]).wait()
    both = jnp.concatenate([ag8[...].reshape(n_y * 8, 256), ag1[...].reshape(n_y, 256)], axis=0)
    high = both.astype(BF16)
    low = (both - high.astype(F32)).astype(BF16)
    chosen = jnp.dot(high, hot, preferred_element_type=F32) + jnp.dot(
        low, hot, preferred_element_type=F32
    )
    total = jnp.zeros((8, 384), F32)
    for at, (o, i) in enumerate(PLACES):
        total = total + jnp.where(source == 4 * o + i, chosen[8 * at : 8 * at + 8], 0.0)
    last = chosen[8 * n_y : 9 * n_y]
    cc[0, 0:8] = total
    cc[0, 8:9] = jnp.sum(
        jnp.where(place_source == source, last, 0.0),
        axis=0, keepdims=True,
    )

    for side, (there, _, row) in enumerate(y_sides):

        def own_row(side=side):
            yrecv[side, 0:12] = ysend[side, 0:12]

        arrived(there, yrecv.at[side], h_recv.at[side], own_row)
    for side, (there, _, x) in enumerate(x_sides):
        row = 9 + 2 * side
        for which in range(2):
            cc[0, row + which : row + which + 1, 0:256] = yrecv[which, x : x + 1]
    for (there, _, _), copy in zip(x_sides, coarse):
        send(there, [copy])

    def onto_lanes(which):
        for rows, to in ((slice(0, 8), s8), (slice(8, 9), s1)):
            for i in range(3):
                pair = spread(cc[which, rows, 128 * i : 128 * i + 128])
                for j in range(2):
                    to[which, :, 128 * (2 * i + j) : 128 * (2 * i + j + 1)] = pair[j]

    sub = lax.broadcasted_iota(jnp.int32, (8, 128), 0)

    def hat_rows(at, element):
        t = at.astype(F32) * 0.25 + (0.125 - 0.5)
        return jnp.maximum(1.0 - jnp.abs(t - element), 0.0)

    tile0 = [hat_rows(sub, e - 1) for e in range(4)]
    tile1 = [hat_rows(sub + 8, e + 1) for e in range(4)]

    def along_y(which, k):
        rows = []
        for e in range(6):
            lanes = slice(128 * e, 128 * e + 128)
            row = s8[which, k : k + 1, lanes] if k < 8 else s1[which, :, lanes]
            rows.append(jnp.broadcast_to(row, (8, 128)))
        return (
            sum(tile0[i] * rows[i] for i in range(4)),
            sum(tile1[i] * rows[i + 2] for i in range(4)),
            jnp.where(
                (sub & 2) == 0, 0.625 * rows[0] + 0.375 * rows[1], 0.625 * rows[5] + 0.375 * rows[4]
            ),
        )

    onto_lanes(0)
    for k in range(9):
        for i, value in enumerate(along_y(0, k)):
            mid[k, i] = value
    for half in range(2):
        crs[half, 9 * HALF :] = jnp.zeros((8, 128), F32)
        rows = [yrecv[which, at + 2 * half : at + 2 * half + 2] for at in (4, 8) for which in range(2)]
        f = fibers(
            jnp.concatenate([rows[0], rows[1]] * 2, axis=0), jnp.concatenate([rows[2], rows[3]] * 2, axis=0)
        )
        for i in range(3):
            fib[i, HALF * half + 48 : HALF * half + 56] = f[i]
    row_iota = lax.broadcasted_iota(jnp.int32, (16, 256), 0)
    lane = lax.broadcasted_iota(jnp.int32, (16, 256), 1)

    def from_below(a, edge):
        return jnp.where(row_iota == 0, edge, pltpu.roll(a, 1, 0))

    def from_above(a, edge):
        return jnp.where(row_iota == 15, edge, pltpu.roll(a, 15, 0))

    def onward(a):
        return pltpu.roll(a, 255, 1)

    def z_slope(v):
        at = lax.broadcasted_iota(jnp.int32, v.shape, 1)
        after = jnp.where(at == 255, v, pltpu.roll(v, 255, 1))
        before = jnp.where(at == 0, v, pltpu.roll(v, 1, 1))
        return after - before

    def flux(d1, step, d2, s2, d3, s3):
        return 0.5 * (d1 * step + 0.25 * (d2 * s2 + d3 * s3))

    XX, YY, ZZ, XY, XZ, YZ = range(6)

    def plane(i, p):
        return con[i, plane_row(p) : plane_row(p) + 16]

    ends = ((0, 0, first_y), (1, 15, last_y))
    for which, row, outside in ends:
        vh[which] = jnp.zeros((8, 256), F32)
        for x in range(4):
            vh[which, x + 1 : x + 2] = jnp.where(outside, pot[x, row : row + 1], yrecv[which, x : x + 1])

    def halves(sequence):
        slope_y, slope_z = [None] * 6, [None] * 6
        for half in sequence:
            there, _, x = x_sides[half]

            def own_plane(half=half, x=x):
                beside_x[half, 0] = pot[x]
                beside_x[half, 1:3] = ang[:, x]

            def own_elements(half=half):
                cc[1 + half] = cc[0]
                for which in range(2):
                    row = 11 - 2 * half + which
                    cc[1 + half, row : row + 1] = cc[0, 9 + 2 * half + which : 10 + 2 * half + which]

            arrived(there, beside_x.at[half], p_recv.at[half], own_plane)
            f = fibers(beside_x[half, 1], beside_x[half, 2])
            outer_p = 5 * half
            for i in range(3):
                fib[i, plane_row(outer_p) : plane_row(outer_p) + 16] = f[i]
            arrived(there, cc.at[1 + half], c_recv.at[half], own_elements)

            onto_lanes(1 + half)
            t = hat_rows((sub & 1) + 2 * half, 0), hat_rows((sub & 1) + 2 * half, 2 * half - 1)
            weights = ((0.625, 0.375), (0.375, 0.625), (0.125, 0.875))
            for k in range(9):
                side = along_y(1 + half, k)
                base = HALF * k
                for number, (a, b) in enumerate(weights[:: 1 - 2 * half]):
                    for i in range(2):
                        at = base + 16 * number + 8 * i
                        crs[half, at : at + 8] = a * side[i] + b * mid[k, i]
                crs[half, base + 48 : base + 56] = t[0] * mid[k, 2] + t[1] * side[2]
            c = crs[half]
            rest = c - c.astype(BF16).astype(F32)
            left = lax.broadcasted_iota(jnp.int32, c.shape, 1) < 64
            fine[half] = jnp.dot(
                jnp.where(left, c, rest).astype(BF16), hat, preferred_element_type=F32
            )
            for tile in range(7):
                at = 8 * tile
                row = HALF * half + at
                f = [fine[half, HALF * k + at : HALF * k + at + 8] for k in range(9)]
                fiber = [fib[i, row : row + 8] for i in range(3)]
                inside = (2 <= tile < 6) if half == 0 else tile < 4
                d, length = tensor_rows(f, fiber, inside)
                for i in range(6):
                    con[i, row : row + 8] = d[i]
                if inside:
                    stretch[row : row + 8] = length

            for which, row, outside in ends:
                corner = cc[1 + half, 11 - 2 * half + which : 12 - 2 * half + which, 0:256]
                vh[which, outer_p : outer_p + 1] = jnp.where(outside, beside_x[half, 0, row : row + 1], corner)
            volt = [beside_x[0, 0]] + [pot[x] for x in range(4)] + [beside_x[1, 0]]
            edge_z = [z_slope(vh[which]) for which in range(2)]
            for p in range(3 * half, 3 * half + 3):
                slope_y[p] = from_above(volt[p], vh[1, p : p + 1]) - from_below(volt[p], vh[0, p : p + 1])
                slope_z[p] = z_slope(volt[p])

            def across(p):
                return flux(
                    plane(XX, p) + plane(XX, p + 1), volt[p + 1] - volt[p],
                    plane(XY, p) + plane(XY, p + 1), slope_y[p] + slope_y[p + 1],
                    plane(XZ, p) + plane(XZ, p + 1), slope_z[p] + slope_z[p + 1],
                )

            def within(x):
                p = x + 1
                v = volt[p]
                slope_x = volt[p + 1] - volt[p - 1]
                d_xy, d_yy, d_yz = plane(XY, p), plane(YY, p), plane(YZ, p)
                faces = []
                for which, shift in ((0, from_below), (1, from_above)):
                    row = beside_row(x, which)
                    step = shift(v, vh[which, p : p + 1])
                    step = v - step if which == 0 else step - v
                    faces.append(
                        flux(
                            d_yy + shift(d_yy, con[YY, row : row + 1]), step,
                            d_xy + shift(d_xy, con[XY, row : row + 1]),
                            slope_x + shift(slope_x, vh[which, p + 1 : p + 2] - vh[which, p - 1 : p]),
                            d_yz + shift(d_yz, con[YZ, row : row + 1]),
                            slope_z[p] + shift(slope_z[p], edge_z[which][p : p + 1]),
                        )
                    )
                faces[0] = jnp.where((row_iota == 0) & first_y, 0.0, faces[0])
                faces[1] = jnp.where((row_iota == 15) & last_y, 0.0, faces[1])
                d_xz, d_zz = plane(XZ, p), plane(ZZ, p)
                upper = flux(
                    d_zz + onward(d_zz), onward(v) - v,
                    d_xz + onward(d_xz), slope_x + onward(slope_x),
                    d_yz + onward(d_yz), slope_y[p] + onward(slope_y[p]),
                )
                upper = jnp.where(lane == 255, 0.0, upper)
                w = rec[x]
                current = excite_gain * v * (v - excite_level) * (v - 1.0) + v * w
                long = jnp.maximum(stretch[plane_row(p) : plane_row(p) + 16] - 1.0, 0.0)
                current = current + stretch_gain * long * (v - stretch_reversal)
                divergent = (faces[1] - faces[0]) + (upper - pltpu.roll(upper, 1, 1))
                return v + time_step * (divergent - current)

            if half == 0:
                face = across(1)
                onev[0] = within(0) + time_step * (face - jnp.where(first_x, 0.0, across(0)))
                onev[1] = within(1) - time_step * face
            else:
                face = across(3)
                onev[2] = within(2) + time_step * face
                onev[3] = within(3) + time_step * (jnp.where(last_x, 0.0, across(4)) - face)
            if half == sequence[1]:
                middle = time_step * across(2)
                onev[1] = onev[1] + middle
                onev[2] = onev[2] - middle

    upper_first = jnp.logical_or(late, gx == 1)

    @pl.when(upper_first)
    def _():
        halves((1, 0))

    @pl.when(jnp.logical_not(upper_first))
    def _():
        halves((0, 1))

    whole(ag8.at[1:n_y], g_send.at[0]).wait()
    whole(ag1.at[1:n_y], g_send.at[1]).wait()
    for side, (there, _, _) in enumerate(y_sides):
        sent(there, srecv.at[side], s_send.at[side])
        sent(there, yrecv.at[side], h_send.at[side])
    for side, (there, _, _) in enumerate(x_sides):
        sent(there, beside_x.at[side], p_send.at[side])
        sent(there, cc.at[1 + side], c_send.at[side])


def store(pot, rec, pot_out, rec_out, sem):
    copies = [pltpu.make_async_copy(a, b, sem.at[i]) for i, (a, b) in enumerate(((pot, pot_out), (rec, rec_out)))]
    for copy in copies:
        copy.start()
    for copy in copies:
        copy.wait()


def make_local(n_x, n_y):
    assert n_y == 16

    def local(potential, recovery, fiber_angles, deform, elem_slot):
        anywhere = pl.BlockSpec(memory_space=pl.ANY)
        cells = (4, 16, 256)
        dma = pltpu.SemaphoreType.DMA
        call = pl.pallas_call(
            lambda *refs: kernel(n_x, n_y, *refs),
            out_shape=(jax.ShapeDtypeStruct(cells, F32),) * 2,
            in_specs=[pl.BlockSpec(memory_space=pltpu.HBM)] * 5,
            out_specs=(pl.BlockSpec(memory_space=pltpu.VMEM),) * 2,
            scratch_shapes=[
                pltpu.VMEM(cells, F32),
                pltpu.VMEM(cells, F32),
                pltpu.VMEM((2,) + cells, F32),
                pltpu.VMEM((4, 64), jnp.int32),
                pltpu.VMEM((9, 256), F32),
                pltpu.VMEM((n_y, 8, 256), F32),
                pltpu.VMEM((n_y, 1, 256), F32),
                pltpu.VMEM((2, 16, 256), F32),
                pltpu.VMEM((2, 16, 256), F32),
                pltpu.VMEM((2, 4, 64), jnp.int32),
                pltpu.VMEM((2, 3, 16, 256), F32),
                pltpu.VMEM((3, 16, 384), F32),
                pltpu.VMEM((3, 8, 768), F32),
                pltpu.VMEM((3, 1, 768), F32),
                pltpu.VMEM((3, ROWS, 256), F32),
                pltpu.VMEM((9, 3, 8, 128), F32),
                pltpu.VMEM((2, 9 * HALF + 8, 128), F32),
                pltpu.VMEM((2, 9 * HALF + 8, 256), F32),
                pltpu.VMEM((6, ROWS, 256), F32),
                pltpu.VMEM((ROWS, 256), F32),
                pltpu.VMEM((2, 8, 256), F32),
                dma((5,)),
                dma((2,)),
                dma((5, 2)),
                dma((2,)),
                dma((2,)),
                dma((2,)),
                dma((2,)),
                dma((2,)),
                dma((2,)),
                dma((2,)),
                dma((2,)),
            ],
            compiler_params=pltpu.CompilerParams(
                collective_id=0, has_side_effects=True, vmem_limit_bytes=16 * 2**20
            ),
            name="step",
        )
        args = (potential, recovery, fiber_angles, deform, elem_slot.reshape(4, 64))
        held = call(*(pltpu.with_memory_space_constraint(a, pltpu.HBM) for a in args))
        return pl.pallas_call(
            store,
            out_shape=(jax.ShapeDtypeStruct(cells, F32),) * 2,
            in_specs=[pl.BlockSpec(memory_space=pltpu.VMEM)] * 2,
            out_specs=(anywhere, anywhere),
            scratch_shapes=[dma((2,))],
            compiler_params=pltpu.CompilerParams(vmem_limit_bytes=16 * 2**20),
            name="store",
        )(*held)

    return local


def solution(mesh):
    placed = (
        P("gx", "gy", None),
        P("gx", "gy", None),
        P(None, "gx", "gy", None),
        P(None, ("gx", "gy")),
        P("gx", "gy", None),
    )
    return jax.shard_map(
        make_local(mesh.shape["gx"], mesh.shape["gy"]),
        mesh=mesh,
        in_specs=placed,
        out_specs=(P("gx", "gy", None), P("gx", "gy", None)),
        check_vma=False,
    )
```

```python
import jax
import jax.numpy as jnp
from jax import lax
from jax.experimental import pallas as pl
from jax.experimental.pallas import tpu as pltpu
from jax.sharding import PartitionSpec as P

sigma_fiber = 1.0
sigma_cross = 0.3
time_step = 0.1
excite_gain = 8.0
excite_level = 0.15
stretch_gain = 10.0
stretch_reversal = 0.6
recover_rate = 0.5

MESH = pl.DeviceIdType.MESH
F32 = jnp.float32
BF16 = jnp.bfloat16

HALF = 56
ROWS = 112


def plane_row(p):
    return 16 * p if p < 3 else HALF + 16 * (p - 3)


def beside_row(x, which):
    return 48 + HALF * (x // 2) + 2 * which + x % 2


def sin_cos(angle):
    half = 0.5 * angle
    sq = half * half
    s = -2.5052108e-08
    for c in (2.7557319e-06, -1.9841270e-04, 8.3333333e-03, -1.6666667e-01, 1.0):
        s = s * sq + c
    s = s * half
    c2 = 2.0876757e-09
    for c in (-2.7557319e-07, 2.4801587e-05, -1.3888889e-03, 4.1666667e-02, -0.5, 1.0):
        c2 = c2 * sq + c
    return 2.0 * s * c2, 1.0 - 2.0 * s * s


def fibers(azimuth, elevation):
    sin_a, cos_a = sin_cos(azimuth)
    sin_e, cos_e = sin_cos(elevation)
    return cos_a * cos_e, sin_a * cos_e, sin_e


def tensor_rows(f, fiber, want_stretch, entries):
    def el(i, j):
        return f[3 * (i % 3) + j % 3]

    cof = [
        [el(i + 1, j + 1) * el(i + 2, j + 2) - el(i + 1, j + 2) * el(i + 2, j + 1) for j in range(3)]
        for i in range(3)
    ]
    det = el(0, 0) * cof[0][0] + el(0, 1) * cof[0][1] + el(0, 2) * cof[0][2]
    inv = 1.0 / det
    scale = inv * inv
    stretch = None
    if want_stretch:
        st = [el(i, 0) * fiber[0] + el(i, 1) * fiber[1] + el(i, 2) * fiber[2] for i in range(3)]
        stretch = jnp.sqrt(st[0] * st[0] + st[1] * st[1] + st[2] * st[2])
    pulled = [cof[0][i] * fiber[0] + cof[1][i] * fiber[1] + cof[2][i] * fiber[2] for i in range(3)]
    out = {}
    cross_scale, fiber_scale = sigma_cross * scale, (sigma_fiber - sigma_cross) * scale
    scaled = [p * fiber_scale for p in pulled]
    for number in entries:
        a, b = ((0, 0), (1, 1), (2, 2), (0, 1), (0, 2), (1, 2))[number]
        metric = cof[0][a] * cof[0][b] + cof[1][a] * cof[1][b] + cof[2][a] * cof[2][b]
        out[number] = cross_scale * metric + scaled[a] * pulled[b]
    return out, stretch


STRAIGHT = ((1, 0), (2, 0), (3, 0), (1, 1), (1, 3), (3, 1), (3, 3))
COLUMN = ((0, 1), (0, 3), (0, 2))
RELAYED = ((2, 1), (2, 3), (1, 2), (2, 2), (3, 2))
PLACES = ((0, 0),) + STRAIGHT + COLUMN + RELAYED


def spread(pair):
    other = pltpu.roll(pair, 64, 1)
    left = lax.broadcasted_iota(jnp.int32, pair.shape, 1) < 64
    return jnp.where(left, pair, other), jnp.where(left, other, pair)


def kernel(
    n_x, n_y,
    pot_in, rec_in, ang_in, def_in, slot_in, onev, onew,
    pot, rec, ang, slot, dfm, ag8, ag1, ysend, yrecv, srecv, beside_x, cs, cr, s8, s1,
    fib, mid, crs, fine, con, stretch, vh,
    in_sem, g_send, g_recv, s_send, s_recv, h_send, h_recv, p_send, p_recv, c_send, c_recv,
):
    gx = lax.axis_index("gx")
    gy = lax.axis_index("gy")
    first_x, last_x, first_y, last_y = gx == 0, gx == n_x - 1, gy == 0, gy == n_y - 1
    x_sides = ((jnp.logical_not(first_x), (gx - 1, gy), 0), (jnp.logical_not(last_x), (gx + 1, gy), 3))
    y_sides = ((jnp.logical_not(first_y), (gx, gy - 1), 0), (jnp.logical_not(last_y), (gx, gy + 1), 15))
    my_o, my_i = lax.div(gy, 4), lax.rem(gy, 4)

    def peer(o, i):
        return (gx, lax.rem(my_o + o, 4) * 4 + lax.rem(my_i + i, 4))

    direct = ((0, 2), (0, 1), (0, 3), (1, 1), (1, 3), (3, 1), (3, 3), (2, 0), (1, 0), (3, 0))
    every = (
        (2, 2), (1, 2), (3, 2), (0, 2), (2, 1), (2, 3), (1, 1), (1, 3), (3, 1), (3, 3),
        (0, 1), (0, 3), (2, 0), (1, 0), (3, 0),
    )
    late = lax.rem(gx, 2) == 0

    loads = [
        pltpu.make_async_copy(src, dst, in_sem.at[i])
        for i, (src, dst) in enumerate(
            ((def_in, dfm), (slot_in, slot), (pot_in, pot), (ang_in, ang), (rec_in, rec))
        )
    ]
    loads[0].start()
    barrier = pltpu.get_barrier_semaphore()
    for steps in direct:
        pl.semaphore_signal(barrier, inc=1, device_id=peer(*steps), device_id_type=MESH)

    @pl.when(late)
    def _():
        for steps in RELAYED:
            pl.semaphore_signal(barrier, inc=1, device_id=peer(*steps), device_id_type=MESH)

    count = len(direct) + jnp.where(late, len(RELAYED), 0)
    for there, device, *_ in x_sides:

        @pl.when(there)
        def _(device=device):
            pl.semaphore_signal(barrier, inc=1, device_id=device, device_id_type=MESH)

        count += jnp.where(there, 1, 0)

    for load in loads[1:]:
        load.start()
    loads[0].wait()
    ag8[0] = dfm[0:8]
    ag1[0] = dfm[8:9]
    for load in loads[1:]:
        load.wait()
    for side, (_, _, row) in enumerate(y_sides):
        ysend[side, 0:4] = pot[:, row, :]
        ysend[side, 4:8] = ang[0, :, row, :]
        ysend[side, 8:12] = ang[1, :, row, :]
    pl.semaphore_wait(barrier, count)

    def remote(src, dst, send_sem, recv_sem, device):
        return pltpu.make_async_remote_copy(
            src_ref=src, dst_ref=dst, send_sem=send_sem, recv_sem=recv_sem,
            device_id=device, device_id_type=MESH,
        )

    def send(there, copies):
        @pl.when(there)
        def _():
            for copy in copies:
                copy.start()

    def whole(ref, semaphore):
        return pltpu.make_async_copy(ref, ref, semaphore)

    def arrived(there, ref, semaphore, otherwise):
        @pl.when(there)
        def _():
            whole(ref, semaphore).wait()

        @pl.when(jnp.logical_not(there))
        def _():
            otherwise()

    def sent(there, ref, semaphore):
        @pl.when(there)
        def _():
            whole(ref, semaphore).wait()

    def piece(place, steps, device, group):
        return [
            remote(ref.at[place], ref.at[PLACES.index(steps)], g_send.at[k], g_recv.at[group, k], device)
            for k, ref in enumerate((ag8, ag1))
        ]

    def gather(steps):
        group = 1 + COLUMN.index(steps) if steps in COLUMN else 4 if steps in RELAYED else 0
        for copy in piece(0, steps, peer(*steps), group):
            copy.start()

    def relay(steps):
        at, group = PLACES.index(steps), 1 + COLUMN.index(steps)
        for k, ref in enumerate((ag8, ag1)):
            whole(ref.at[at], g_recv.at[group, k]).wait()

        @pl.when(jnp.logical_not(late))
        def _():
            for o in (2, 1, 3):
                to = (o, steps[1])
                for copy in piece(at, to, peer(o, 0), 4 if to in RELAYED else 0):
                    copy.start()

    slots, halos, planes, coarse = [], [], [], []
    for side, (_, device, _) in enumerate(y_sides):
        slots.append(remote(slot, srecv.at[1 - side], s_send.at[side], s_recv.at[1 - side], device))
        halos.append(remote(ysend.at[side], yrecv.at[1 - side], h_send.at[side], h_recv.at[1 - side], device))
    for side, (_, device, x) in enumerate(x_sides):
        planes.append(
            [
                remote(
                    pot.at[x] if i == 0 else ang.at[i - 1, x], beside_x.at[1 - side, i],
                    p_send.at[side], p_recv.at[1 - side], device,
                )
                for i in range(3)
            ]
        )
        coarse.append(remote(cs.at[side], cr.at[1 - side], c_send.at[side], c_recv.at[1 - side], device))
    for (there, _, _), copy in zip(y_sides, slots):
        send(there, [copy])

    @pl.when(late)
    def _():
        for steps in every:
            gather(steps)

    @pl.when(jnp.logical_not(late))
    def _():
        for steps in direct:
            if 0 in steps:
                gather(steps)

    for (there, _, _), copy in zip(y_sides, halos):
        send(there, [copy])
    for (there, _, _), copies in zip(x_sides, planes):
        send(there, copies)

    for side in range(2):
        cs[side, :, 384:512] = jnp.zeros((8, 128), F32)
    for x in range(4):
        v, w = pot[x], rec[x]
        onew[x] = w + time_step * recover_rate * (
            -w - excite_gain * v * (v - excite_level - 1.0)
        )
        f = fibers(ang[0, x], ang[1, x])
        for i in range(3):
            fib[i, plane_row(x + 1) : plane_row(x + 1) + 16] = f[i]

    k_iota = lax.broadcasted_iota(jnp.int32, (128, 256), 0) & 63
    z_iota = lax.broadcasted_iota(jnp.int32, (128, 256), 1)
    place = jnp.clip((z_iota.astype(F32) + 0.5) * 0.25 - 0.5, 0.0, 63.0)
    hat = jnp.maximum(1.0 - jnp.abs(place - k_iota.astype(F32)), 0.0).astype(BF16)

    relay((0, 1))
    relay((0, 3))

    for side, (there, _, _) in enumerate(y_sides):

        def own_slots(side=side):
            srecv[side] = slot[...]

        arrived(there, srecv.at[side], s_recv.at[side], own_slots)
    mine = slot[...]
    below = jnp.where(first_y, mine[0:1], srecv[0, 3:4])
    above = jnp.where(last_y, mine[3:4], srecv[1, 0:1])
    wanted = jnp.concatenate(
        [below, mine[0:1], mine[1:2], mine[2:3], mine[3:4], above], axis=1
    )
    local = wanted & 255
    source = (((my_o - (wanted >> 10)) & 3) << 2) | ((my_i - (wanted >> 8)) & 3)
    place_iota = lax.broadcasted_iota(jnp.int32, (n_y, 384), 0)
    place_source = sum(jnp.where(place_iota == at, 4 * o + i, 0) for at, (o, i) in enumerate(PLACES))
    hot = jnp.where(
        lax.broadcasted_iota(jnp.int32, (256, 384), 0) == local, 1.0, 0.0
    ).astype(BF16)

    relay((0, 2))

    for k, ref in enumerate((ag8, ag1)):
        whole(ref.at[1:8], g_recv.at[0, k]).wait()
        whole(ref.at[11:16], g_recv.at[4, k]).wait()
    both = jnp.concatenate([ag8[...].reshape(n_y * 8, 256), ag1[...].reshape(n_y, 256)], axis=0)
    high = both.astype(BF16)
    low = (both - high.astype(F32)).astype(BF16)
    chosen = jnp.dot(high, hot, preferred_element_type=F32) + jnp.dot(
        low, hot, preferred_element_type=F32
    )
    total = jnp.zeros((8, 384), F32)
    for at, (o, i) in enumerate(PLACES):
        total = total + jnp.where(source == 4 * o + i, chosen[8 * at : 8 * at + 8], 0.0)
    last = chosen[8 * n_y : 9 * n_y]
    ninth = jnp.sum(
        jnp.where(place_source == source, last, 0.0),
        axis=0, keepdims=True,
    )
    for side in range(2):
        cs[side, :, 0:384] = total
        for i in range(3):
            cs[side, i : i + 1, 384:512] = ninth[:, 128 * i : 128 * i + 128]

    for side, (there, _, row) in enumerate(y_sides):

        def own_row(side=side):
            yrecv[side, 0:12] = ysend[side, 0:12]

        arrived(there, yrecv.at[side], h_recv.at[side], own_row)
    for side, (there, _, x) in enumerate(x_sides):
        for which in range(2):
            for i in range(2):
                row = 3 + 2 * which + i
                cs[side, row : row + 1, 384:512] = yrecv[which, x : x + 1, 128 * i : 128 * i + 128]
    for (there, _, _), copy in zip(x_sides, coarse):
        send(there, [copy])

    def onto_lanes(which):
        held, at = (cr, which - 1) if which else (cs, 0)
        for i in range(3):
            pairs = spread(held[at, :, 128 * i : 128 * i + 128]), spread(held[at, i : i + 1, 384:512])
            for to, pair in zip((s8, s1), pairs):
                for j in range(2):
                    to[which, :, 128 * (2 * i + j) : 128 * (2 * i + j + 1)] = pair[j]

    sub = lax.broadcasted_iota(jnp.int32, (8, 128), 0)

    def hat_rows(at, element):
        t = at.astype(F32) * 0.25 + (0.125 - 0.5)
        return jnp.maximum(1.0 - jnp.abs(t - element), 0.0)

    tile0 = [hat_rows(sub, e - 1) for e in range(4)]
    tile1 = [hat_rows(sub + 8, e + 1) for e in range(4)]

    def along_y(which, k):
        rows = []
        for e in range(6):
            lanes = slice(128 * e, 128 * e + 128)
            row = s8[which, k : k + 1, lanes] if k < 8 else s1[which, :, lanes]
            rows.append(jnp.broadcast_to(row, (8, 128)))
        return (
            sum(tile0[i] * rows[i] for i in range(4)),
            sum(tile1[i] * rows[i + 2] for i in range(4)),
            jnp.where(
                (sub & 2) == 0, 0.625 * rows[0] + 0.375 * rows[1], 0.625 * rows[5] + 0.375 * rows[4]
            ),
        )

    onto_lanes(0)
    for k in range(9):
        for i, value in enumerate(along_y(0, k)):
            mid[k, i] = value
    for half in range(2):
        crs[half, 9 * HALF :] = jnp.zeros((8, 128), F32)
        rows = [yrecv[which, at + 2 * half : at + 2 * half + 2] for at in (4, 8) for which in range(2)]
        f = fibers(
            jnp.concatenate([rows[0], rows[1]] * 2, axis=0), jnp.concatenate([rows[2], rows[3]] * 2, axis=0)
        )
        for i in range(3):
            fib[i, HALF * half + 48 : HALF * half + 56] = f[i]
    row_iota = lax.broadcasted_iota(jnp.int32, (16, 256), 0)
    lane = lax.broadcasted_iota(jnp.int32, (16, 256), 1)

    def from_below(a, edge):
        return jnp.where(row_iota == 0, edge, pltpu.roll(a, 1, 0))

    def from_above(a, edge):
        return jnp.where(row_iota == 15, edge, pltpu.roll(a, 15, 0))

    def onward(a):
        return pltpu.roll(a, 255, 1)

    def z_slope(v):
        at = lax.broadcasted_iota(jnp.int32, v.shape, 1)
        after = jnp.where(at == 255, v, pltpu.roll(v, 255, 1))
        before = jnp.where(at == 0, v, pltpu.roll(v, 1, 1))
        return after - before

    def flux(d1, step, d2, s2, d3, s3):
        return 0.5 * (d1 * step + 0.25 * (d2 * s2 + d3 * s3))

    XX, YY, ZZ, XY, XZ, YZ = range(6)

    def plane(i, p):
        return con[i, plane_row(p) : plane_row(p) + 16]

    ends = ((0, 0, first_y), (1, 15, last_y))
    for which, row, outside in ends:
        vh[which] = jnp.zeros((8, 256), F32)
        for x in range(4):
            vh[which, x + 1 : x + 2] = jnp.where(outside, pot[x, row : row + 1], yrecv[which, x : x + 1])

    def halves(sequence):
        slope_y, slope_z = [None] * 6, [None] * 6
        for half in sequence:
            there, _, x = x_sides[half]

            def own_plane(half=half, x=x):
                beside_x[half, 0] = pot[x]
                beside_x[half, 1:3] = ang[:, x]

            def own_elements(half=half):
                cr[half] = cs[half]

            arrived(there, beside_x.at[half], p_recv.at[half], own_plane)
            f = fibers(beside_x[half, 1], beside_x[half, 2])
            outer_p = 5 * half
            for i in range(3):
                fib[i, plane_row(outer_p) : plane_row(outer_p) + 16] = f[i]
            arrived(there, cr.at[half], c_recv.at[half], own_elements)

            onto_lanes(1 + half)
            t = hat_rows((sub & 1) + 2 * half, 0), hat_rows((sub & 1) + 2 * half, 2 * half - 1)
            weights = ((0.625, 0.375), (0.375, 0.625), (0.125, 0.875))
            for k in range(9):
                side = along_y(1 + half, k)
                base = HALF * k
                for number, (a, b) in enumerate(weights[:: 1 - 2 * half]):
                    for i in range(2):
                        at = base + 16 * number + 8 * i
                        crs[half, at : at + 8] = a * side[i] + b * mid[k, i]
                crs[half, base + 48 : base + 56] = t[0] * mid[k, 2] + t[1] * side[2]
            c = crs[half]
            rest = c - c.astype(BF16).astype(F32)
            left = lax.broadcasted_iota(jnp.int32, c.shape, 1) < 64
            fine[half] = jnp.dot(
                jnp.where(left, c, rest).astype(BF16), hat, preferred_element_type=F32
            )
            for tile in range(7):
                at = 8 * tile
                row = HALF * half + at
                f = [fine[half, HALF * k + at : HALF * k + at + 8] for k in range(9)]
                fiber = [fib[i, row : row + 8] for i in range(3)]
                inside = (2 <= tile < 6) if half == 0 else tile < 4
                entries = range(6) if inside else (YY, XY, YZ) if tile == 6 else (XX, XY, XZ)
                d, length = tensor_rows(f, fiber, inside, entries)
                for i in entries:
                    con[i, row : row + 8] = d[i]
                if inside:
                    stretch[row : row + 8] = length

            for which, row, outside in ends:
                corner = jnp.concatenate(
                    [cr[half, 3 + 2 * which + i : 4 + 2 * which + i, 384:512] for i in range(2)], axis=1
                )
                vh[which, outer_p : outer_p + 1] = jnp.where(outside, beside_x[half, 0, row : row + 1], corner)
            volt = [beside_x[0, 0]] + [pot[x] for x in range(4)] + [beside_x[1, 0]]
            edge_z = [z_slope(vh[which]) for which in range(2)]
            for p in range(3 * half, 3 * half + 3):
                slope_y[p] = from_above(volt[p], vh[1, p : p + 1]) - from_below(volt[p], vh[0, p : p + 1])
                slope_z[p] = z_slope(volt[p])

            def across(p):
                return flux(
                    plane(XX, p) + plane(XX, p + 1), volt[p + 1] - volt[p],
                    plane(XY, p) + plane(XY, p + 1), slope_y[p] + slope_y[p + 1],
                    plane(XZ, p) + plane(XZ, p + 1), slope_z[p] + slope_z[p + 1],
                )

            def within(x):
                p = x + 1
                v = volt[p]
                slope_x = volt[p + 1] - volt[p - 1]
                d_xy, d_yy, d_yz = plane(XY, p), plane(YY, p), plane(YZ, p)
                faces = []
                for which, shift in ((0, from_below), (1, from_above)):
                    row = beside_row(x, which)
                    step = shift(v, vh[which, p : p + 1])
                    step = v - step if which == 0 else step - v
                    faces.append(
                        flux(
                            d_yy + shift(d_yy, con[YY, row : row + 1]), step,
                            d_xy + shift(d_xy, con[XY, row : row + 1]),
                            slope_x + shift(slope_x, vh[which, p + 1 : p + 2] - vh[which, p - 1 : p]),
                            d_yz + shift(d_yz, con[YZ, row : row + 1]),
                            slope_z[p] + shift(slope_z[p], edge_z[which][p : p + 1]),
                        )
                    )
                faces[0] = jnp.where((row_iota == 0) & first_y, 0.0, faces[0])
                faces[1] = jnp.where((row_iota == 15) & last_y, 0.0, faces[1])
                d_xz, d_zz = plane(XZ, p), plane(ZZ, p)
                upper = flux(
                    d_zz + onward(d_zz), onward(v) - v,
                    d_xz + onward(d_xz), slope_x + onward(slope_x),
                    d_yz + onward(d_yz), slope_y[p] + onward(slope_y[p]),
                )
                upper = jnp.where(lane == 255, 0.0, upper)
                w = rec[x]
                current = excite_gain * v * (v - excite_level) * (v - 1.0) + v * w
                long = jnp.maximum(stretch[plane_row(p) : plane_row(p) + 16] - 1.0, 0.0)
                current = current + stretch_gain * long * (v - stretch_reversal)
                divergent = (faces[1] - faces[0]) + (upper - pltpu.roll(upper, 1, 1))
                return v + time_step * (divergent - current)

            if half == 0:
                face = across(1)
                onev[0] = within(0) + time_step * (face - jnp.where(first_x, 0.0, across(0)))
                onev[1] = within(1) - time_step * face
            else:
                face = across(3)
                onev[2] = within(2) + time_step * face
                onev[3] = within(3) + time_step * (jnp.where(last_x, 0.0, across(4)) - face)
            if half == sequence[1]:
                middle = time_step * across(2)
                onev[1] = onev[1] + middle
                onev[2] = onev[2] - middle

    upper_first = jnp.logical_or(late, gx == 1)

    @pl.when(upper_first)
    def _():
        halves((1, 0))

    @pl.when(jnp.logical_not(upper_first))
    def _():
        halves((0, 1))

    whole(ag8.at[1:n_y], g_send.at[0]).wait()
    whole(ag1.at[1:n_y], g_send.at[1]).wait()
    for side, (there, _, _) in enumerate(y_sides):
        sent(there, srecv.at[side], s_send.at[side])
        sent(there, yrecv.at[side], h_send.at[side])
    for side, (there, _, _) in enumerate(x_sides):
        sent(there, beside_x.at[side], p_send.at[side])
        sent(there, cr.at[side], c_send.at[side])


def store(pot, rec, pot_out, rec_out, sem):
    copies = [pltpu.make_async_copy(a, b, sem.at[i]) for i, (a, b) in enumerate(((pot, pot_out), (rec, rec_out)))]
    for copy in copies:
        copy.start()
    for copy in copies:
        copy.wait()


def make_local(n_x, n_y):
    assert n_y == 16

    def local(potential, recovery, fiber_angles, deform, elem_slot):
        anywhere = pl.BlockSpec(memory_space=pl.ANY)
        cells = (4, 16, 256)
        dma = pltpu.SemaphoreType.DMA
        call = pl.pallas_call(
            lambda *refs: kernel(n_x, n_y, *refs),
            out_shape=(jax.ShapeDtypeStruct(cells, F32),) * 2,
            in_specs=[pl.BlockSpec(memory_space=pltpu.HBM)] * 5,
            out_specs=(pl.BlockSpec(memory_space=pltpu.VMEM),) * 2,
            scratch_shapes=[
                pltpu.VMEM(cells, F32),
                pltpu.VMEM(cells, F32),
                pltpu.VMEM((2,) + cells, F32),
                pltpu.VMEM((4, 64), jnp.int32),
                pltpu.VMEM((9, 256), F32),
                pltpu.VMEM((n_y, 8, 256), F32),
                pltpu.VMEM((n_y, 1, 256), F32),
                pltpu.VMEM((2, 16, 256), F32),
                pltpu.VMEM((2, 16, 256), F32),
                pltpu.VMEM((2, 4, 64), jnp.int32),
                pltpu.VMEM((2, 3, 16, 256), F32),
                pltpu.VMEM((2, 8, 512), F32),
                pltpu.VMEM((2, 8, 512), F32),
                pltpu.VMEM((3, 8, 768), F32),
                pltpu.VMEM((3, 1, 768), F32),
                pltpu.VMEM((3, ROWS, 256), F32),
                pltpu.VMEM((9, 3, 8, 128), F32),
                pltpu.VMEM((2, 9 * HALF + 8, 128), F32),
                pltpu.VMEM((2, 9 * HALF + 8, 256), F32),
                pltpu.VMEM((6, ROWS, 256), F32),
                pltpu.VMEM((ROWS, 256), F32),
                pltpu.VMEM((2, 8, 256), F32),
                dma((5,)),
                dma((2,)),
                dma((5, 2)),
                dma((2,)),
                dma((2,)),
                dma((2,)),
                dma((2,)),
                dma((2,)),
                dma((2,)),
                dma((2,)),
                dma((2,)),
            ],
            compiler_params=pltpu.CompilerParams(
                collective_id=0, has_side_effects=True, vmem_limit_bytes=16 * 2**20
            ),
            name="step",
        )
        args = (potential, recovery, fiber_angles, deform, elem_slot.reshape(4, 64))
        held = call(*(pltpu.with_memory_space_constraint(a, pltpu.HBM) for a in args))
        return pl.pallas_call(
            store,
            out_shape=(jax.ShapeDtypeStruct(cells, F32),) * 2,
            in_specs=[pl.BlockSpec(memory_space=pltpu.VMEM)] * 2,
            out_specs=(anywhere, anywhere),
            scratch_shapes=[dma((2,))],
            compiler_params=pltpu.CompilerParams(vmem_limit_bytes=16 * 2**20),
            name="store",
        )(*held)

    return local


def solution(mesh):
    placed = (
        P("gx", "gy", None),
        P("gx", "gy", None),
        P(None, "gx", "gy", None),
        P(None, ("gx", "gy")),
        P("gx", "gy", None),
    )
    return jax.shard_map(
        make_local(mesh.shape["gx"], mesh.shape["gy"]),
        mesh=mesh,
        in_specs=placed,
        out_specs=(P("gx", "gy", None), P("gx", "gy", None)),
        check_vma=False,
    )
```

```python
import jax
import jax.numpy as jnp
from jax import lax
from jax.experimental import pallas as pl
from jax.experimental.pallas import tpu as pltpu
from jax.sharding import PartitionSpec as P

sigma_fiber = 1.0
sigma_cross = 0.3
time_step = 0.1
excite_gain = 8.0
excite_level = 0.15
stretch_gain = 10.0
stretch_reversal = 0.6
recover_rate = 0.5

MESH = pl.DeviceIdType.MESH
F32 = jnp.float32
BF16 = jnp.bfloat16

HALF = 56
ROWS = 112


def plane_row(p):
    return 16 * p if p < 3 else HALF + 16 * (p - 3)


def beside_row(x, which):
    return 48 + HALF * (x // 2) + 2 * which + x % 2


def sin_cos(angle):
    half = 0.5 * angle
    sq = half * half
    s = -2.5052108e-08
    for c in (2.7557319e-06, -1.9841270e-04, 8.3333333e-03, -1.6666667e-01, 1.0):
        s = s * sq + c
    s = s * half
    c2 = 2.0876757e-09
    for c in (-2.7557319e-07, 2.4801587e-05, -1.3888889e-03, 4.1666667e-02, -0.5, 1.0):
        c2 = c2 * sq + c
    return 2.0 * s * c2, 1.0 - 2.0 * s * s


def fibers(azimuth, elevation):
    sin_a, cos_a = sin_cos(azimuth)
    sin_e, cos_e = sin_cos(elevation)
    return cos_a * cos_e, sin_a * cos_e, sin_e


def tensor_rows(f, fiber, want_stretch, entries):
    def el(i, j):
        return f[3 * (i % 3) + j % 3]

    cof = [
        [el(i + 1, j + 1) * el(i + 2, j + 2) - el(i + 1, j + 2) * el(i + 2, j + 1) for j in range(3)]
        for i in range(3)
    ]
    det = el(0, 0) * cof[0][0] + el(0, 1) * cof[0][1] + el(0, 2) * cof[0][2]
    inv = 1.0 / det
    scale = inv * inv
    stretch = None
    if want_stretch:
        st = [el(i, 0) * fiber[0] + el(i, 1) * fiber[1] + el(i, 2) * fiber[2] for i in range(3)]
        stretch = jnp.sqrt(st[0] * st[0] + st[1] * st[1] + st[2] * st[2])
    pulled = [cof[0][i] * fiber[0] + cof[1][i] * fiber[1] + cof[2][i] * fiber[2] for i in range(3)]
    out = {}
    cross_scale, fiber_scale = sigma_cross * scale, (sigma_fiber - sigma_cross) * scale
    scaled = [p * fiber_scale for p in pulled]
    for number in entries:
        a, b = ((0, 0), (1, 1), (2, 2), (0, 1), (0, 2), (1, 2))[number]
        metric = cof[0][a] * cof[0][b] + cof[1][a] * cof[1][b] + cof[2][a] * cof[2][b]
        out[number] = cross_scale * metric + scaled[a] * pulled[b]
    return out, stretch


STRAIGHT = ((1, 0), (2, 0), (3, 0), (1, 1), (1, 3), (3, 1), (3, 3))
COLUMN = ((0, 1), (0, 3), (0, 2))
RELAYED = ((2, 1), (2, 3), (1, 2), (2, 2), (3, 2))
PLACES = ((0, 0),) + STRAIGHT + COLUMN + RELAYED


def spread(pair):
    other = pltpu.roll(pair, 64, 1)
    left = lax.broadcasted_iota(jnp.int32, pair.shape, 1) < 64
    return jnp.where(left, pair, other), jnp.where(left, other, pair)


def kernel(
    n_x, n_y,
    pot_in, rec_in, ang_in, def_in, slot_in, onev, onew,
    pot, rec, ang, slot, dfm, ag8, ag1, ysend, yrecv, srecv, beside_x, cs, cr, s8, s1,
    fib, mid, crs, fine, con, stretch, vh,
    in_sem, g_send, g_recv, s_send, s_recv, h_send, h_recv, p_send, p_recv, c_send, c_recv,
):
    gx = lax.axis_index("gx")
    gy = lax.axis_index("gy")
    first_x, last_x, first_y, last_y = gx == 0, gx == n_x - 1, gy == 0, gy == n_y - 1
    x_sides = ((jnp.logical_not(first_x), (gx - 1, gy), 0), (jnp.logical_not(last_x), (gx + 1, gy), 3))
    y_sides = ((jnp.logical_not(first_y), (gx, gy - 1), 0), (jnp.logical_not(last_y), (gx, gy + 1), 15))
    my_o, my_i = lax.div(gy, 4), lax.rem(gy, 4)

    def peer(o, i):
        return (gx, lax.rem(my_o + o, 4) * 4 + lax.rem(my_i + i, 4))

    direct = ((0, 2), (0, 1), (0, 3), (1, 1), (1, 3), (3, 1), (3, 3), (2, 0), (1, 0), (3, 0))
    every = (
        (2, 2), (1, 2), (3, 2), (0, 2), (2, 1), (2, 3), (1, 1), (1, 3), (3, 1), (3, 3),
        (0, 1), (0, 3), (2, 0), (1, 0), (3, 0),
    )
    late = lax.rem(gx, 2) == 0

    loads = [
        pltpu.make_async_copy(src, dst, in_sem.at[i])
        for i, (src, dst) in enumerate(
            ((def_in, dfm), (slot_in, slot), (pot_in, pot), (ang_in, ang), (rec_in, rec))
        )
    ]
    loads[0].start()
    barrier = pltpu.get_barrier_semaphore()
    for steps in direct:
        pl.semaphore_signal(barrier, inc=1, device_id=peer(*steps), device_id_type=MESH)

    @pl.when(late)
    def _():
        for steps in RELAYED:
            pl.semaphore_signal(barrier, inc=1, device_id=peer(*steps), device_id_type=MESH)

    count = len(direct) + jnp.where(late, len(RELAYED), 0)
    for there, device, *_ in x_sides:

        @pl.when(there)
        def _(device=device):
            pl.semaphore_signal(barrier, inc=1, device_id=device, device_id_type=MESH)

        count += jnp.where(there, 1, 0)

    for load in loads[1:]:
        load.start()
    loads[0].wait()
    ag8[0] = dfm[0:8]
    ag1[0] = dfm[8:9]
    for load in loads[1:]:
        load.wait()
    for side, (_, _, row) in enumerate(y_sides):
        ysend[side, 0:4] = pot[:, row, :]
        ysend[side, 4:8] = ang[0, :, row, :]
        ysend[side, 8:12] = ang[1, :, row, :]
    pl.semaphore_wait(barrier, count)

    def remote(src, dst, send_sem, recv_sem, device):
        return pltpu.make_async_remote_copy(
            src_ref=src, dst_ref=dst, send_sem=send_sem, recv_sem=recv_sem,
            device_id=device, device_id_type=MESH,
        )

    def send(there, copies):
        @pl.when(there)
        def _():
            for copy in copies:
                copy.start()

    def whole(ref, semaphore):
        return pltpu.make_async_copy(ref, ref, semaphore)

    def arrived(there, ref, semaphore, otherwise):
        @pl.when(there)
        def _():
            whole(ref, semaphore).wait()

        @pl.when(jnp.logical_not(there))
        def _():
            otherwise()

    def sent(there, ref, semaphore):
        @pl.when(there)
        def _():
            whole(ref, semaphore).wait()

    def piece(place, steps, device, group):
        return [
            remote(ref.at[place], ref.at[PLACES.index(steps)], g_send.at[k], g_recv.at[group, k], device)
            for k, ref in enumerate((ag8, ag1))
        ]

    def gather(steps):
        group = 1 + COLUMN.index(steps) if steps in COLUMN else 4 if steps in RELAYED else 0
        for copy in piece(0, steps, peer(*steps), group):
            copy.start()

    def relay(steps):
        at, group = PLACES.index(steps), 1 + COLUMN.index(steps)
        for k, ref in enumerate((ag8, ag1)):
            whole(ref.at[at], g_recv.at[group, k]).wait()

        @pl.when(jnp.logical_not(late))
        def _():
            for o in (2, 1, 3):
                to = (o, steps[1])
                for copy in piece(at, to, peer(o, 0), 4 if to in RELAYED else 0):
                    copy.start()

    slots, halos, planes, coarse = [], [], [], []
    for side, (_, device, _) in enumerate(y_sides):
        slots.append(remote(slot, srecv.at[1 - side], s_send.at[side], s_recv.at[1 - side], device))
        halos.append(remote(ysend.at[side], yrecv.at[1 - side], h_send.at[side], h_recv.at[1 - side], device))
    for side, (_, device, x) in enumerate(x_sides):
        planes.append(
            [
                remote(
                    pot.at[x] if i == 0 else ang.at[i - 1, x], beside_x.at[1 - side, i],
                    p_send.at[side], p_recv.at[1 - side], device,
                )
                for i in range(3)
            ]
        )
        coarse.append(remote(cs.at[side], cr.at[1 - side], c_send.at[side], c_recv.at[1 - side], device))
    for (there, _, _), copy in zip(y_sides, slots):
        send(there, [copy])

    @pl.when(late)
    def _():
        for steps in every:
            gather(steps)

    @pl.when(jnp.logical_not(late))
    def _():
        for steps in direct:
            if 0 in steps:
                gather(steps)

    for (there, _, _), copy in zip(y_sides, halos):
        send(there, [copy])
    for (there, _, _), copies in zip(x_sides, planes):
        send(there, copies)

    for side in range(2):
        cs[side, :, 384:512] = jnp.zeros((8, 128), F32)
    for x in range(4):
        v, w = pot[x], rec[x]
        onew[x] = w + time_step * recover_rate * (
            -w - excite_gain * v * (v - excite_level - 1.0)
        )
        f = fibers(ang[0, x], ang[1, x])
        for i in range(3):
            fib[i, plane_row(x + 1) : plane_row(x + 1) + 16] = f[i]

    k_iota = lax.broadcasted_iota(jnp.int32, (128, 256), 0) & 63
    z_iota = lax.broadcasted_iota(jnp.int32, (128, 256), 1)
    place = jnp.clip((z_iota.astype(F32) + 0.5) * 0.25 - 0.5, 0.0, 63.0)
    hat = jnp.maximum(1.0 - jnp.abs(place - k_iota.astype(F32)), 0.0).astype(BF16)

    relay((0, 1))
    relay((0, 3))

    for side, (there, _, _) in enumerate(y_sides):

        def own_slots(side=side):
            srecv[side] = slot[...]

        arrived(there, srecv.at[side], s_recv.at[side], own_slots)
    mine = slot[...]
    below = jnp.where(first_y, mine[0:1], srecv[0, 3:4])
    above = jnp.where(last_y, mine[3:4], srecv[1, 0:1])
    wanted = jnp.concatenate(
        [below, mine[0:1], mine[1:2], mine[2:3], mine[3:4], above], axis=1
    )
    local = wanted & 255
    source = (((my_o - (wanted >> 10)) & 3) << 2) | ((my_i - (wanted >> 8)) & 3)
    place_iota = lax.broadcasted_iota(jnp.int32, (n_y, 384), 0)
    place_source = sum(jnp.where(place_iota == at, 4 * o + i, 0) for at, (o, i) in enumerate(PLACES))
    hot = jnp.where(
        lax.broadcasted_iota(jnp.int32, (256, 384), 0) == local, 1.0, 0.0
    ).astype(BF16)

    relay((0, 2))

    for k, ref in enumerate((ag8, ag1)):
        whole(ref.at[1:8], g_recv.at[0, k]).wait()
        whole(ref.at[11:16], g_recv.at[4, k]).wait()
    both = jnp.concatenate([ag8[...].reshape(n_y * 8, 256), ag1[...].reshape(n_y, 256)], axis=0)
    high = both.astype(BF16)
    low = (both - high.astype(F32)).astype(BF16)
    chosen = jnp.dot(high, hot, preferred_element_type=F32) + jnp.dot(
        low, hot, preferred_element_type=F32
    )
    total = jnp.zeros((8, 384), F32)
    for at, (o, i) in enumerate(PLACES):
        total = total + jnp.where(source == 4 * o + i, chosen[8 * at : 8 * at + 8], 0.0)
    last = chosen[8 * n_y : 9 * n_y]
    ninth = jnp.sum(
        jnp.where(place_source == source, last, 0.0),
        axis=0, keepdims=True,
    )
    for side in range(2):
        cs[side, :, 0:384] = total
        for i in range(3):
            cs[side, i : i + 1, 384:512] = ninth[:, 128 * i : 128 * i + 128]

    for side, (there, _, row) in enumerate(y_sides):

        def own_row(side=side):
            yrecv[side, 0:12] = ysend[side, 0:12]

        arrived(there, yrecv.at[side], h_recv.at[side], own_row)
    for side, (there, _, x) in enumerate(x_sides):
        for which in range(2):
            for i in range(2):
                row = 3 + 2 * which + i
                cs[side, row : row + 1, 384:512] = yrecv[which, x : x + 1, 128 * i : 128 * i + 128]
    for (there, _, _), copy in zip(x_sides, coarse):
        send(there, [copy])

    def onto_lanes(which):
        held, at = (cr, which - 1) if which else (cs, 0)
        for i in range(3):
            pairs = spread(held[at, :, 128 * i : 128 * i + 128]), spread(held[at, i : i + 1, 384:512])
            for to, pair in zip((s8, s1), pairs):
                for j in range(2):
                    to[which, :, 128 * (2 * i + j) : 128 * (2 * i + j + 1)] = pair[j]

    sub = lax.broadcasted_iota(jnp.int32, (8, 128), 0)

    def hat_rows(at, element):
        t = at.astype(F32) * 0.25 + (0.125 - 0.5)
        return jnp.maximum(1.0 - jnp.abs(t - element), 0.0)

    tile0 = [hat_rows(sub, e - 1) for e in range(4)]
    tile1 = [hat_rows(sub + 8, e + 1) for e in range(4)]

    def along_y(which, k):
        rows = []
        for e in range(6):
            lanes = slice(128 * e, 128 * e + 128)
            row = s8[which, k : k + 1, lanes] if k < 8 else s1[which, :, lanes]
            rows.append(jnp.broadcast_to(row, (8, 128)))
        return (
            sum(tile0[i] * rows[i] for i in range(4)),
            sum(tile1[i] * rows[i + 2] for i in range(4)),
            jnp.where(
                (sub & 2) == 0, 0.625 * rows[0] + 0.375 * rows[1], 0.625 * rows[5] + 0.375 * rows[4]
            ),
        )

    onto_lanes(0)
    for k in range(9):
        for i, value in enumerate(along_y(0, k)):
            mid[k, i] = value
    for half in range(2):
        crs[half, 9 * HALF :] = jnp.zeros((8, 128), F32)
        rows = [yrecv[which, at + 2 * half : at + 2 * half + 2] for at in (4, 8) for which in range(2)]
        f = fibers(
            jnp.concatenate([rows[0], rows[1]] * 2, axis=0), jnp.concatenate([rows[2], rows[3]] * 2, axis=0)
        )
        for i in range(3):
            fib[i, HALF * half + 48 : HALF * half + 56] = f[i]
    row_iota = lax.broadcasted_iota(jnp.int32, (16, 256), 0)
    lane = lax.broadcasted_iota(jnp.int32, (16, 256), 1)

    def from_below(a, edge):
        return jnp.where(row_iota == 0, edge, pltpu.roll(a, 1, 0))

    def from_above(a, edge):
        return jnp.where(row_iota == 15, edge, pltpu.roll(a, 15, 0))

    def onward(a):
        return pltpu.roll(a, 255, 1)

    def z_slope(v):
        at = lax.broadcasted_iota(jnp.int32, v.shape, 1)
        after = jnp.where(at == 255, v, pltpu.roll(v, 255, 1))
        before = jnp.where(at == 0, v, pltpu.roll(v, 1, 1))
        return after - before

    def flux(d1, step, d2, s2, d3, s3):
        return 0.5 * (d1 * step + 0.25 * (d2 * s2 + d3 * s3))

    XX, YY, ZZ, XY, XZ, YZ = range(6)

    def plane(i, p):
        return con[i, plane_row(p) : plane_row(p) + 16]

    ends = ((0, 0, first_y), (1, 15, last_y))
    for which, row, outside in ends:
        vh[which] = jnp.zeros((8, 256), F32)
        for x in range(4):
            vh[which, x + 1 : x + 2] = jnp.where(outside, pot[x, row : row + 1], yrecv[which, x : x + 1])

    def halves(sequence):
        slope_y, slope_z = [None] * 6, [None] * 6
        for half in sequence:
            there, _, x = x_sides[half]

            def own_plane(half=half, x=x):
                beside_x[half, 0] = pot[x]
                beside_x[half, 1:3] = ang[:, x]

            def own_elements(half=half):
                cr[half] = cs[half]

            arrived(there, beside_x.at[half], p_recv.at[half], own_plane)
            f = fibers(beside_x[half, 1], beside_x[half, 2])
            outer_p = 5 * half
            for i in range(3):
                fib[i, plane_row(outer_p) : plane_row(outer_p) + 16] = f[i]
            beyond = beside_x[half, 0]
            inner = (1, 2) if half == 0 else (3, 4)
            for p in inner:
                slope_y[p] = from_above(pot[p - 1], vh[1, p : p + 1]) - from_below(pot[p - 1], vh[0, p : p + 1])
                slope_z[p] = z_slope(pot[p - 1])
            slope_z[outer_p] = z_slope(beyond)
            arrived(there, cr.at[half], c_recv.at[half], own_elements)

            onto_lanes(1 + half)
            t = hat_rows((sub & 1) + 2 * half, 0), hat_rows((sub & 1) + 2 * half, 2 * half - 1)
            weights = ((0.625, 0.375), (0.375, 0.625), (0.125, 0.875))
            for k in range(9):
                side = along_y(1 + half, k)
                base = HALF * k
                for number, (a, b) in enumerate(weights[:: 1 - 2 * half]):
                    for i in range(2):
                        at = base + 16 * number + 8 * i
                        crs[half, at : at + 8] = a * side[i] + b * mid[k, i]
                crs[half, base + 48 : base + 56] = t[0] * mid[k, 2] + t[1] * side[2]
            c = crs[half]
            rest = c - c.astype(BF16).astype(F32)
            left = lax.broadcasted_iota(jnp.int32, c.shape, 1) < 64
            fine[half] = jnp.dot(
                jnp.where(left, c, rest).astype(BF16), hat, preferred_element_type=F32
            )
            for tile in range(7):
                at = 8 * tile
                row = HALF * half + at
                f = [fine[half, HALF * k + at : HALF * k + at + 8] for k in range(9)]
                fiber = [fib[i, row : row + 8] for i in range(3)]
                inside = (2 <= tile < 6) if half == 0 else tile < 4
                entries = range(6) if inside else (YY, XY, YZ) if tile == 6 else (XX, XY, XZ)
                d, length = tensor_rows(f, fiber, inside, entries)
                for i in entries:
                    con[i, row : row + 8] = d[i]
                if inside:
                    stretch[row : row + 8] = length

            for which, row, outside in ends:
                corner = jnp.concatenate(
                    [cr[half, 3 + 2 * which + i : 4 + 2 * which + i, 384:512] for i in range(2)], axis=1
                )
                vh[which, outer_p : outer_p + 1] = jnp.where(outside, beside_x[half, 0, row : row + 1], corner)
            volt = [beside_x[0, 0]] + [pot[x] for x in range(4)] + [beside_x[1, 0]]
            edge_z = [z_slope(vh[which]) for which in range(2)]
            above, below = (vh[which, outer_p : outer_p + 1] for which in (1, 0))
            slope_y[outer_p] = from_above(beyond, above) - from_below(beyond, below)

            def across(p):
                return flux(
                    plane(XX, p) + plane(XX, p + 1), volt[p + 1] - volt[p],
                    plane(XY, p) + plane(XY, p + 1), slope_y[p] + slope_y[p + 1],
                    plane(XZ, p) + plane(XZ, p + 1), slope_z[p] + slope_z[p + 1],
                )

            def within(x):
                p = x + 1
                v = volt[p]
                slope_x = volt[p + 1] - volt[p - 1]
                d_xy, d_yy, d_yz = plane(XY, p), plane(YY, p), plane(YZ, p)
                faces = []
                for which, shift in ((0, from_below), (1, from_above)):
                    row = beside_row(x, which)
                    step = shift(v, vh[which, p : p + 1])
                    step = v - step if which == 0 else step - v
                    faces.append(
                        flux(
                            d_yy + shift(d_yy, con[YY, row : row + 1]), step,
                            d_xy + shift(d_xy, con[XY, row : row + 1]),
                            slope_x + shift(slope_x, vh[which, p + 1 : p + 2] - vh[which, p - 1 : p]),
                            d_yz + shift(d_yz, con[YZ, row : row + 1]),
                            slope_z[p] + shift(slope_z[p], edge_z[which][p : p + 1]),
                        )
                    )
                faces[0] = jnp.where((row_iota == 0) & first_y, 0.0, faces[0])
                faces[1] = jnp.where((row_iota == 15) & last_y, 0.0, faces[1])
                d_xz, d_zz = plane(XZ, p), plane(ZZ, p)
                upper = flux(
                    d_zz + onward(d_zz), onward(v) - v,
                    d_xz + onward(d_xz), slope_x + onward(slope_x),
                    d_yz + onward(d_yz), slope_y[p] + onward(slope_y[p]),
                )
                upper = jnp.where(lane == 255, 0.0, upper)
                w = rec[x]
                current = excite_gain * v * (v - excite_level) * (v - 1.0) + v * w
                long = jnp.maximum(stretch[plane_row(p) : plane_row(p) + 16] - 1.0, 0.0)
                current = current + stretch_gain * long * (v - stretch_reversal)
                divergent = (faces[1] - faces[0]) + (upper - pltpu.roll(upper, 1, 1))
                return v + time_step * (divergent - current)

            if half == 0:
                face = across(1)
                onev[0] = within(0) + time_step * (face - jnp.where(first_x, 0.0, across(0)))
                onev[1] = within(1) - time_step * face
            else:
                face = across(3)
                onev[2] = within(2) + time_step * face
                onev[3] = within(3) + time_step * (jnp.where(last_x, 0.0, across(4)) - face)
            if half == sequence[1]:
                middle = time_step * across(2)
                onev[1] = onev[1] + middle
                onev[2] = onev[2] - middle

    upper_first = jnp.logical_or(late, gx == 1)

    @pl.when(upper_first)
    def _():
        halves((1, 0))

    @pl.when(jnp.logical_not(upper_first))
    def _():
        halves((0, 1))

    whole(ag8.at[1:n_y], g_send.at[0]).wait()
    whole(ag1.at[1:n_y], g_send.at[1]).wait()
    for side, (there, _, _) in enumerate(y_sides):
        sent(there, srecv.at[side], s_send.at[side])
        sent(there, yrecv.at[side], h_send.at[side])
    for side, (there, _, _) in enumerate(x_sides):
        sent(there, beside_x.at[side], p_send.at[side])
        sent(there, cr.at[side], c_send.at[side])


def store(pot, rec, pot_out, rec_out, sem):
    copies = [pltpu.make_async_copy(a, b, sem.at[i]) for i, (a, b) in enumerate(((pot, pot_out), (rec, rec_out)))]
    for copy in copies:
        copy.start()
    for copy in copies:
        copy.wait()


def make_local(n_x, n_y):
    assert n_y == 16

    def local(potential, recovery, fiber_angles, deform, elem_slot):
        anywhere = pl.BlockSpec(memory_space=pl.ANY)
        cells = (4, 16, 256)
        dma = pltpu.SemaphoreType.DMA
        call = pl.pallas_call(
            lambda *refs: kernel(n_x, n_y, *refs),
            out_shape=(jax.ShapeDtypeStruct(cells, F32),) * 2,
            in_specs=[pl.BlockSpec(memory_space=pltpu.HBM)] * 5,
            out_specs=(pl.BlockSpec(memory_space=pltpu.VMEM),) * 2,
            scratch_shapes=[
                pltpu.VMEM(cells, F32),
                pltpu.VMEM(cells, F32),
                pltpu.VMEM((2,) + cells, F32),
                pltpu.VMEM((4, 64), jnp.int32),
                pltpu.VMEM((9, 256), F32),
                pltpu.VMEM((n_y, 8, 256), F32),
                pltpu.VMEM((n_y, 1, 256), F32),
                pltpu.VMEM((2, 16, 256), F32),
                pltpu.VMEM((2, 16, 256), F32),
                pltpu.VMEM((2, 4, 64), jnp.int32),
                pltpu.VMEM((2, 3, 16, 256), F32),
                pltpu.VMEM((2, 8, 512), F32),
                pltpu.VMEM((2, 8, 512), F32),
                pltpu.VMEM((3, 8, 768), F32),
                pltpu.VMEM((3, 1, 768), F32),
                pltpu.VMEM((3, ROWS, 256), F32),
                pltpu.VMEM((9, 3, 8, 128), F32),
                pltpu.VMEM((2, 9 * HALF + 8, 128), F32),
                pltpu.VMEM((2, 9 * HALF + 8, 256), F32),
                pltpu.VMEM((6, ROWS, 256), F32),
                pltpu.VMEM((ROWS, 256), F32),
                pltpu.VMEM((2, 8, 256), F32),
                dma((5,)),
                dma((2,)),
                dma((5, 2)),
                dma((2,)),
                dma((2,)),
                dma((2,)),
                dma((2,)),
                dma((2,)),
                dma((2,)),
                dma((2,)),
                dma((2,)),
            ],
            compiler_params=pltpu.CompilerParams(
                collective_id=0, has_side_effects=True, vmem_limit_bytes=16 * 2**20
            ),
            name="step",
        )
        args = (potential, recovery, fiber_angles, deform, elem_slot.reshape(4, 64))
        held = call(*(pltpu.with_memory_space_constraint(a, pltpu.HBM) for a in args))
        return pl.pallas_call(
            store,
            out_shape=(jax.ShapeDtypeStruct(cells, F32),) * 2,
            in_specs=[pl.BlockSpec(memory_space=pltpu.VMEM)] * 2,
            out_specs=(anywhere, anywhere),
            scratch_shapes=[dma((2,))],
            compiler_params=pltpu.CompilerParams(vmem_limit_bytes=16 * 2**20),
            name="store",
        )(*held)

    return local


def solution(mesh):
    placed = (
        P("gx", "gy", None),
        P("gx", "gy", None),
        P(None, "gx", "gy", None),
        P(None, ("gx", "gy")),
        P("gx", "gy", None),
    )
    return jax.shard_map(
        make_local(mesh.shape["gx"], mesh.shape["gy"]),
        mesh=mesh,
        in_specs=placed,
        out_specs=(P("gx", "gy", None), P("gx", "gy", None)),
        check_vma=False,
    )
```
